32 devices in a mesh: seq: 8 (over z, y), head: 4 (over x, core).
Axes of the slice: x: 2, y: 2, z: 4, core: 2. Of those that a mesh axis runs over, the one named last changes fastest.
Arguments:
- byte_input: float32 [3072, 2048], P('seq', 'head'), may hold values from -6 to 6
- b_proj: float32 [3072, 128], P('seq'), may hold values from -1.25 to 1.25
- c_proj: float32 [3072, 128], P('seq'), may hold values from -1.25 to 1.25
- step_decay: float32 [32, 3072], P('head', 'seq'), may hold values from 0 to 1
- skip_gain: float32 [32], P('head'), may hold values from 0.5 to 1.5
- out_weight: bfloat16 [2048, 1024], P('head'), may hold values from -0.125 to 0.125
- boundaries: int32 [8, 128], P('seq'), may hold values from 0 to 383, as said below
- counts: int32 [8], P('seq'), may hold values from 0 to 128, as said below
- norm_gain: float32 [1024], replicated, may hold values from 0.1 to 1.9
- qkv_weight: bfloat16 [3, 1024, 2048], P(None, None, 'head'), may hold values from -1 to 1
Outputs:
- attended: float32 [512, 2048], P('seq', 'head')
The draws below stay inside these ranges and needn't reach their ends.
Inputs may be any that keep to these rules, and one draw needn't show every extreme that they name: `boundaries`: row s holds counts[s] strictly increasing offsets, then zeros. The counts sum to 512; for every shard s the sum of the counts of shards before s lies within 32 of s * 64; some shard has 128.
All inputs are finite; a program needn't handle non-finite values.
Results may differ from the reference program's by a relative error of at most 0.0075.
Values may be sent and summed in bfloat16 or wider, within the bound.
A program may use at most 128 MiB of HBM per device.

```python
import jax
import jax.numpy as jnp
from jax import lax

D_ENC = 1024
RECURRENT_LANES = 32
STATE = 128
ATT_DIM = 64
BYTES_DEV = 384
ROWS_DEV = 64
D_INNER = 2048
D_MAIN = 2048
SLOTS = 128
SHARDS = 8
TOTAL_BYTES = 3072
COARSE = 512


def draw_step_decay(key, part):
    matched_entries = jax.random.split(jax.random.fold_in(key, 11), 7)
    share = 0.5
    fast = jax.random.uniform(matched_entries[0], (RECURRENT_LANES,)) < share
    fast_rate = jnp.exp(jax.random.uniform(matched_entries[1], (RECURRENT_LANES,), minval=jnp.log(1.0 / 50.0), maxval=jnp.log(1.0 / 30.0)))
    slow_rate = jax.random.uniform(matched_entries[2], (RECURRENT_LANES,), minval=0.3, maxval=0.6) / TOTAL_BYTES
    starting_shift = jnp.where(fast, fast_rate, slow_rate)
    partition_factor = jnp.exp(jax.random.uniform(matched_entries[3], (RECURRENT_LANES, SHARDS), minval=jnp.log(0.5), maxval=jnp.log(2.0)))
    partition_factor = jnp.repeat(partition_factor, BYTES_DEV, axis=1)
    approximate_guess = jax.random.uniform(matched_entries[4], (RECURRENT_LANES, TOTAL_BYTES), minval=0.5, maxval=1.5)
    destination_spots = jax.random.randint(matched_entries[5], (RECURRENT_LANES, 3), 0, TOTAL_BYTES)
    contiguous_extent = jax.random.uniform(matched_entries[6], (RECURRENT_LANES, 3), minval=0.22, maxval=0.69)
    entry_position = jnp.arange(TOTAL_BYTES)
    contiguous_bundles = jnp.sum(jnp.where(entry_position[None, None, :] == destination_spots[:, :, None], contiguous_extent[:, :, None], 0.0), axis=1)
    return (starting_shift[:, None] * partition_factor * approximate_guess + contiguous_bundles).astype(jnp.float32)


def boundary_plan(key):
    matched_entries = jax.random.split(jax.random.fold_in(key, 5), 3)
    half = ROWS_DEV // 2
    drift = jax.random.randint(matched_entries[0], (SHARDS,), -half, half + 1)
    summit = jax.random.randint(matched_entries[1], (), 1, SHARDS - 1)
    index = jnp.arange(SHARDS)
    drift = jnp.where(index == summit - 1, -half, drift)
    drift = jnp.where(index == summit, half, drift)
    drift = jnp.where(index == SHARDS - 1, 0, drift)
    before = jnp.concatenate([jnp.zeros((1,), drift.dtype), drift[:-1]])
    number = ROWS_DEV + drift - before
    orders = jax.vmap(lambda piece_key: jax.random.permutation(piece_key, BYTES_DEV))(jax.random.split(matched_entries[2], SHARDS))
    slot = jnp.arange(SLOTS)
    chosen = jnp.where(slot[None, :] < number[:, None], orders[:, :SLOTS], BYTES_DEV)
    chosen = jnp.sort(chosen, axis=1)
    chosen = jnp.where(slot[None, :] < number[:, None], chosen, 0)
    return (number.astype(jnp.int32), chosen.astype(jnp.int32))


def draw_counts(key, part):
    return boundary_plan(key)[0]


def draw_boundaries(key, part):
    return boundary_plan(key)[1]


def draw_qkv_weight(key, part):
    matched_entries = jax.random.split(jax.random.fold_in(key, 23), 1)
    spread = D_ENC ** (-0.5)
    drawn = jnp.clip(jax.random.normal(matched_entries[0], (3, D_ENC, D_MAIN)), -4.0, 4.0) * spread
    return jnp.clip(drawn, -1.0, 1.0).astype(jnp.bfloat16)


def block_levels(key, shape, cuts, least, top_value):
    factor_of, own = 1.0, jax.random.fold_in(key, 6)
    for dim, blocks in cuts:
        draws = jnp.exp(jax.random.uniform(jax.random.fold_in(own, dim), (blocks,), jnp.float32, least / len(cuts), top_value / len(cuts)))
        factor_of = factor_of * jnp.repeat(draws, shape[dim] // blocks).reshape([-1 if axis == dim else 1 for axis in range(len(shape))])
    return factor_of


def noise(key, dims, scale, reach, cuts=(), kind=jnp.bfloat16):
    values = scale * jax.random.normal(key, dims, jnp.float32)
    if cuts:
        values = values * block_levels(key, dims, cuts, -0.22, 0.18)
    return jnp.clip(values, -reach, reach).astype(kind)


def setup_inputs(seed: int = 0) -> dict:
    seeds = jax.random.split(jax.random.key(seed), 11)
    byte_input = noise(seeds[0], (TOTAL_BYTES, D_INNER), 1.0, 6.0, ((0, 8), (1, 4)), jnp.float32)
    b_proj = noise(seeds[1], (TOTAL_BYTES, STATE), (STATE ** -0.5), 1.25, ((0, 8),), jnp.float32)
    c_proj = noise(seeds[2], (TOTAL_BYTES, STATE), (STATE ** -0.5), 1.25, ((0, 8),), jnp.float32)
    step_decay = draw_step_decay(jax.random.fold_in(seeds[10], 71), 0)
    skip_gain = jnp.clip(0.5 + 1.0 * jax.random.uniform(seeds[4], (RECURRENT_LANES,), jnp.float32) ** block_levels(seeds[4], (RECURRENT_LANES,), ((0, 4),), -0.2, 0.2), 0.5, 1.5)
    out_weight = noise(seeds[5], (D_INNER, D_ENC), D_INNER ** -0.5, 0.125, ((0, 4),))
    boundaries = draw_boundaries(jax.random.fold_in(seeds[10], 71), 0)
    counts = draw_counts(jax.random.fold_in(seeds[10], 71), 0)
    norm_gain = jnp.clip(1.0 + 0.18 * jax.random.normal(seeds[8], (D_ENC,), jnp.float32), 0.1, 1.9)
    qkv_weight = draw_qkv_weight(jax.random.fold_in(seeds[10], 71), 0)
    return {"byte_input": byte_input, "b_proj": b_proj, "c_proj": c_proj, "step_decay": step_decay, "skip_gain": skip_gain, "out_weight": out_weight, "boundaries": boundaries, "counts": counts, "norm_gain": norm_gain, "qkv_weight": qkv_weight}


def state_space(inputs, b_rows, c_rows, decay):
    log_decay = jnp.cumsum(-decay, axis=1)
    affinity = jnp.dot(c_rows, b_rows.T, precision=lax.Precision.HIGHEST)
    length = inputs.shape[0]
    causal = lax.broadcasted_iota(jnp.int32, (length, length), 0) >= lax.broadcasted_iota(jnp.int32, (length, length), 1)

    def one_head(pair):
        values, logs = pair
        weights = jnp.where(causal, jnp.exp(jnp.where(causal, logs[:, None] - logs[None, :], 0.0)), 0.0) * affinity
        return jnp.dot(weights, values, precision=lax.Precision.HIGHEST)
    inside = lax.map(one_head, (inputs.transpose(1, 0, 2), log_decay))
    tail = jnp.exp(log_decay[:, -1:] - log_decay)
    own_state = jnp.einsum('ht,thp,tn->hpn', tail, inputs, b_rows, precision=lax.Precision.HIGHEST)
    return (log_decay, inside, own_state)

def reference(byte_input, b_proj, c_proj, step_decay, skip_gain, out_weight, boundaries, counts, norm_gain, qkv_weight):
    shards = counts.shape[0]
    heads = step_decay.shape[0]
    inputs = byte_input.reshape(shards, BYTES_DEV, heads, -1)
    b_rows = b_proj.reshape(shards, BYTES_DEV, -1)
    c_rows = c_proj.reshape(shards, BYTES_DEV, -1)
    decays = step_decay.reshape(heads, shards, BYTES_DEV).transpose(1, 0, 2)

    def advance(state, block):
        values, b_block, c_block, decay = block
        log_decay, inside, own_state = state_space(values, b_block, c_block, decay)
        carried = jnp.exp(log_decay)[:, :, None] * jnp.einsum('tn,hpn->htp', c_block, state, precision=lax.Precision.HIGHEST)
        mixed_heads = inside + carried + skip_gain[:, None, None] * values.transpose(1, 0, 2)
        new_state = jnp.exp(log_decay[:, -1])[:, None, None] * state + own_state
        return (new_state, mixed_heads)
    start_state = jnp.zeros((heads, inputs.shape[3], b_proj.shape[1]), jnp.float32)
    _, outputs = lax.scan(advance, start_state, (inputs, b_rows, c_rows, decays))
    y_rows = outputs.transpose(0, 2, 1, 3).reshape(shards * BYTES_DEV, -1).astype(jnp.bfloat16)
    slots = boundaries.shape[1]
    slot = jnp.arange(slots, dtype=jnp.int32)
    valid = slot[None, :] < counts[:, None]
    starts = (jnp.cumsum(counts) - counts).astype(jnp.int32)
    rank = jnp.where(valid, starts[:, None] + slot[None, :], COARSE).astype(jnp.int32)
    destination_spots = (boundaries + (jnp.arange(shards, dtype=jnp.int32) * BYTES_DEV)[:, None]).astype(jnp.int32)
    chosen = jnp.zeros((COARSE,), jnp.int32).at[rank.reshape(-1)].set(destination_spots.reshape(-1), mode='drop')
    rows = jnp.take(y_rows, chosen, axis=0)
    mixed = jnp.dot(rows, out_weight, preferred_element_type=jnp.float32)
    normed = (mixed * lax.rsqrt(lax.optimization_barrier(jnp.mean(mixed * mixed, axis=-1, keepdims=True)) + 1e-05) * norm_gain).astype(jnp.bfloat16)
    query = jnp.dot(normed, qkv_weight[0], preferred_element_type=jnp.float32).astype(jnp.bfloat16)
    keyed = jnp.dot(normed, qkv_weight[1], preferred_element_type=jnp.float32).astype(jnp.bfloat16)
    valued = jnp.dot(normed, qkv_weight[2], preferred_element_type=jnp.float32).astype(jnp.bfloat16)
    total = query.shape[0]
    causal = lax.broadcasted_iota(jnp.int32, (total, total), 0) >= lax.broadcasted_iota(jnp.int32, (total, total), 1)

    def split_heads(matrix):
        return matrix.reshape(total, -1, ATT_DIM).transpose(1, 0, 2)

    def attend(triple):
        q_head, k_head, v_head = triple
        scores = jnp.dot(q_head.astype(jnp.float32), k_head.astype(jnp.float32).T, precision=lax.Precision.HIGHEST) * ATT_DIM ** (-0.5)
        scores = jnp.where(causal, scores, -1e+30)
        highest = lax.optimization_barrier(jnp.max(scores, axis=-1, keepdims=True))
        exps = jnp.where(causal, jnp.exp(scores - highest), 0.0)
        sums = lax.optimization_barrier(jnp.sum(exps, axis=-1, keepdims=True))
        weights = exps.astype(jnp.bfloat16)
        return jnp.dot(weights, v_head, preferred_element_type=jnp.float32) / sums
    result = lax.map(attend, (split_heads(query), split_heads(keyed), split_heads(valued)))
    return result.transpose(1, 0, 2).reshape(total, -1)
```

```python
import functools

import jax
import jax.numpy as jnp
from jax import lax
from jax.experimental import pallas as pl
from jax.experimental.pallas import tpu as pltpu
from jax.sharding import PartitionSpec as P

ATT_DIM = 64
ROWS_DEV = 64


def prefix(shard, axis, combine, identity):
    length, here = (lax.axis_size(axis), lax.axis_index(axis))
    everything = jax.tree.map(lambda part: lax.all_gather(part, axis), shard)
    start = jax.tree.map(
        lambda part, zero: jnp.broadcast_to(jnp.asarray(zero, part.dtype), part.shape),
        shard,
        identity,
    )

    def lap(k, before):
        reached = k < here
        new = combine(before, jax.tree.map(lambda part: part[k], everything))
        return jax.tree.map(lambda a, b: jnp.where(reached, a, b), new, before)

    return lax.fori_loop(0, length, lap, start)


def extended(cells, sides, width):
    for axis, dim in sides:
        count = lax.axis_size(axis)
        ends = count - 1
        head = lax.slice_in_dim(cells, 0, width, axis=dim)
        tail = lax.slice_in_dim(cells, cells.shape[dim] - width, cells.shape[dim], axis=dim)
        cells = jnp.concatenate(
            [
                lax.ppermute(tail, axis, [(i, (i + 1) % count) for i in range(ends)]),
                cells,
                lax.ppermute(head, axis, [((i + 1) % count, i) for i in range(ends)]),
            ],
            axis=dim,
        )
    return cells


def state_space(inputs, b_rows, c_rows, decay):
    log_decay = jnp.cumsum(-decay, axis=1)
    affinity = jnp.dot(c_rows, b_rows.T, precision=lax.Precision.HIGHEST)
    length = inputs.shape[0]
    causal = lax.broadcasted_iota(jnp.int32, (length, length), 0) >= lax.broadcasted_iota(
        jnp.int32, (length, length), 1
    )

    def one_head(pair):
        values, logs = pair
        weights = (
            jnp.where(causal, jnp.exp(jnp.where(causal, logs[:, None] - logs[None, :], 0.0)), 0.0)
            * affinity
        )
        return jnp.dot(weights, values, precision=lax.Precision.HIGHEST)

    inside = lax.map(one_head, (inputs.transpose(1, 0, 2), log_decay))
    tail = jnp.exp(log_decay[:, -1:] - log_decay)
    own_state = jnp.einsum("ht,thp,tn->hpn", tail, inputs, b_rows, precision=lax.Precision.HIGHEST)
    return (log_decay, inside, own_state)


def link(earlier, later):
    return (earlier[0] * later[0], later[0][:, None, None] * earlier[1] + later[1])


def body(
    byte_input,
    b_proj,
    c_proj,
    step_decay,
    skip_gain,
    out_weight,
    boundaries,
    counts,
    norm_gain,
    qkv_weight,
):
    heads_here = step_decay.shape[0]
    length = byte_input.shape[0]
    inputs = byte_input.reshape(length, heads_here, -1)
    log_decay, inside, own_state = state_space(inputs, b_proj, c_proj, step_decay)
    span_decay = jnp.exp(log_decay[:, -1])
    arriving = prefix(
        (span_decay, own_state), "seq", link, (jnp.ones_like(span_decay), jnp.zeros_like(own_state))
    )
    carried = jnp.exp(log_decay)[:, :, None] * jnp.einsum(
        "tn,hpn->htp", c_proj, arriving[1], precision=lax.Precision.HIGHEST
    )
    mixed_heads = inside + carried + skip_gain[:, None, None] * inputs.transpose(1, 0, 2)
    slots = boundaries.shape[1]
    picked = jnp.take(mixed_heads, boundaries[0], axis=1)
    selected = picked.transpose(1, 0, 2).reshape(slots, -1).astype(jnp.bfloat16)
    all_counts = lax.all_gather(counts, "seq", axis=0, tiled=True)
    starts = jnp.cumsum(all_counts) - all_counts
    myself = lax.axis_index("seq")
    shards = lax.axis_size("seq")
    slot = jnp.arange(slots, dtype=jnp.int32)

    def slot_index(source):
        inside_axis = (source >= 0) & (source < shards)
        safe = jnp.clip(source, 0, shards - 1)
        begin = jnp.take(starts, safe)
        number = jnp.take(all_counts, safe)
        return jnp.where(inside_axis & (slot < number), begin + slot, -1)

    global_index = jnp.concatenate(
        [slot_index(myself - 1), slot_index(myself), slot_index(myself + 1)]
    )
    first_row = myself * ROWS_DEV
    target = first_row + jnp.arange(ROWS_DEV, dtype=jnp.int32)
    picker = global_index[None, :] == target[:, None]
    nearby = extended(selected, (("seq", 0),), slots)
    owned = jnp.dot(picker.astype(jnp.bfloat16), nearby, preferred_element_type=jnp.float32).astype(
        jnp.bfloat16
    )
    partial_value = jnp.dot(owned, out_weight, preferred_element_type=jnp.float32)
    packed = lax.psum(partial_value, "head")
    normed = (
        packed * lax.rsqrt(jnp.mean(packed * packed, axis=-1, keepdims=True) + 1e-05) * norm_gain
    ).astype(jnp.bfloat16)
    query = jnp.dot(normed, qkv_weight[0], preferred_element_type=jnp.float32).astype(jnp.bfloat16)
    keyed = jnp.dot(normed, qkv_weight[1], preferred_element_type=jnp.float32).astype(jnp.bfloat16)
    valued = jnp.dot(normed, qkv_weight[2], preferred_element_type=jnp.float32).astype(jnp.bfloat16)
    att_here = query.shape[1] // ATT_DIM
    queries = query.reshape(ROWS_DEV, att_here, ATT_DIM)
    row_place = first_row + jnp.arange(ROWS_DEV, dtype=jnp.int32)
    scale = ATT_DIM ** (-0.5)
    running = jnp.full((att_here, ROWS_DEV), -1e30, jnp.float32)
    key_piece = lax.all_gather(keyed, "seq", axis=0, tiled=True)
    value_piece = lax.all_gather(valued, "seq", axis=0, tiled=True)
    count = key_piece.shape[0]
    key_heads = key_piece.reshape(count, att_here, ATT_DIM)
    value_heads = value_piece.reshape(count, att_here, ATT_DIM)
    scores = (
        jnp.einsum("qhd,khd->hqk", queries, key_heads, preferred_element_type=jnp.float32) * scale
    )
    allowed = jnp.arange(count, dtype=jnp.int32)[None, :] <= row_place[:, None]
    scores = jnp.where(allowed[None], scores, -1e30)
    highest = jnp.maximum(running, jnp.max(scores, axis=-1))
    exps = jnp.where(allowed[None], jnp.exp(scores - highest[:, :, None]), 0.0)
    totals = jnp.sum(exps, axis=-1)
    weights = exps.astype(jnp.bfloat16)
    accum = jnp.einsum("hqk,khd->hqd", weights, value_heads, preferred_element_type=jnp.float32)
    running, totals, accum = (highest, totals, accum)
    result = accum / totals[:, :, None]
    return result.transpose(1, 0, 2).reshape(ROWS_DEV, att_here * ATT_DIM)


F32 = jnp.float32
BF16 = jnp.bfloat16
CHUNKS = 2


def exact_dot(a, b, dims=((1,), (0,))):
    return lax.dot_general(
        a, b, (dims, ((), ())), precision=lax.Precision.HIGHEST, preferred_element_type=F32
    )


def fast_dot(a, b, dims=((1,), (0,))):
    return lax.dot_general(a, b, (dims, ((), ())), preferred_element_type=F32)


def halves(a):
    high = a.astype(BF16)
    return high, (a - high.astype(F32)).astype(BF16)


def iota(shape, dim):
    return lax.broadcasted_iota(jnp.int32, shape, dim)


def fused(
    seqs,
    groups,
    decay_hbm,
    x_hbm,
    b_hbm,
    counts_hbm,
    bound_hbm,
    c_hbm,
    skip_hbm,
    outw_hbm,
    gain_hbm,
    qkvw_hbm,
    out_ref,
    decay_ref,
    x_ref,
    b_ref,
    counts_ref,
    bound_ref,
    c_ref,
    skip_ref,
    outw,
    gain_ref,
    qkvw,
    x_both,
    tag_send,
    tag_recv,
    send_a,
    recv_a,
    send_b,
    recv_b,
    send_p,
    recv_p,
    recv_n,
    send_q,
    recv_q,
    send_o,
    recv_o,
    weight_sem,
    tag_sem,
    a_send,
    a_recv,
    b_send,
    b_recv,
    p_send,
    p_recv,
    n_sem,
    q_send,
    q_recv,
    o_send,
    o_recv,
):
    me = lax.axis_index("seq")
    col = lax.axis_index("head")
    length, width = x_ref.shape
    heads = decay_ref.shape[0]
    lanes = width // heads
    pair_width = 2 * lanes
    pairs = heads // 2
    state = b_ref.shape[1]
    slots = bound_ref.shape[1]
    rows = out_ref.shape[0]
    piece = rows // groups
    half = rows // 2
    lo = (seqs - pairs) // 2
    is_owner = (me >= lo) & (me < lo + pairs)

    def shard_at(d):
        return lax.rem(me + d + seqs, seqs)

    layers = seqs // 2
    mid = layers // 2
    layer, side = me // 2, lax.rem(me, 2)
    near_end = layer < mid
    far_layers = [jnp.where(near_end, layers - 1 - k, k) for k in range(layers - mid)]
    same = jnp.where(near_end, layer, layer - (layers - mid))
    for k in range(1, mid):
        turn = lax.rem(same + k, mid)
        far_layers.append(jnp.where(near_end, turn, turn + (layers - mid)))
    targets = []
    for there in far_layers + [layer]:
        targets.append(2 * there + 1 - side)
        if there is not layer:
            targets.append(2 * there + side)

    def head_at(d):
        return lax.rem(col + d, groups)

    chip = col // 2
    partner = 2 * chip + 1 - lax.rem(col, 2)
    other = 2 * (1 - chip)

    barrier = pltpu.get_barrier_semaphore()
    peers = [(shard_at(d), col) for d in range(1, seqs)]
    peers += [(me, head_at(d)) for d in range(1, groups)]
    peers += [(shard_at(e), head_at(d)) for e in (-1, 1) for d in range(1, groups)]
    for peer in peers:
        pl.semaphore_signal(
            barrier, inc=1, device_id=peer, device_id_type=pl.DeviceIdType.MESH
        )

    def remote(src, dst, send_sem, recv_sem, peer):
        return pltpu.make_async_remote_copy(
            src_ref=src,
            dst_ref=dst,
            send_sem=send_sem,
            recv_sem=recv_sem,
            device_id=peer,
            device_id_type=pl.DeviceIdType.MESH,
        )

    loads = [
        pltpu.make_async_copy(source, target, weight_sem.at[i])
        for i, (source, target) in enumerate(
            (
                (decay_hbm, decay_ref),
                (x_hbm, x_ref),
                (b_hbm, b_ref),
                (counts_hbm, counts_ref),
                (bound_hbm, bound_ref),
                (c_hbm, c_ref),
                (skip_hbm, skip_ref),
                (outw_hbm, outw),
                (gain_hbm, gain_ref),
                (qkvw_hbm, qkvw),
            )
        )
    ]
    for load in loads[:7]:
        load.start()

    loads[0].wait()
    decay = decay_ref[...]
    upper = (iota((length, length), 0) <= iota((length, length), 1)).astype(F32)
    logs = -exact_dot(decay, upper)
    tail = jnp.exp(logs[:, length - 1 : length] - logs)
    loads[3].wait()
    tag_row = iota((heads, state), 1) == iota((heads, state), 0)
    tags = jnp.where(tag_row, logs[:, length - 1 : length], 0.0)
    tags = jnp.sum(tags, axis=0, keepdims=True)
    number = jnp.broadcast_to(counts_ref[...].astype(F32), (1, state))
    tag_send[...] = jnp.where(iota((1, state), 1) == heads, number, tags)
    loads[1].wait()
    loads[2].wait()
    for load in loads[7:]:
        load.start()
    b_turned = b_ref[...].T
    first_half = iota((state, pair_width), 1) < lanes
    for pair in range(pairs):
        x_high, x_low = halves(x_ref[:, pair * pair_width : (pair + 1) * pair_width])
        both = jnp.concatenate([x_high, x_low], axis=1)
        x_both[pair] = both
        faded = [b_turned * tail[h : h + 1, :] for h in (2 * pair, 2 * pair + 1)]
        f_high, f_low = halves(jnp.concatenate(faded, axis=0))
        wide = fast_dot(f_high, both)
        own = wide[:, :pair_width] + wide[:, pair_width:] + fast_dot(f_low, x_high)
        send_a[pair] = jnp.where(first_half, own[:state], own[state:]).astype(BF16)
    pl.semaphore_wait(barrier, len(peers))

    def tag_copy(to, slot, source):
        return remote(tag_send, tag_recv.at[slot], tag_sem.at[0, to], tag_sem.at[1, source], (to, col))

    def a_copy(j, slot):
        return remote(send_a.at[j], recv_a.at[slot], a_send.at[j], a_recv.at[slot], (lo + j, col))

    for to in targets:
        tag_copy(to, me, me).start()
    for k in range(pairs):
        j = jnp.where(near_end, pairs - 1 - k, k)

        @pl.when(me != lo + j)
        def _():
            a_copy(j, me).start()

    tag_recv[me] = tag_send[...]

    @pl.when(is_owner)
    def _():
        recv_a[me] = send_a[me - lo]

    lower = (iota((length, length), 0) >= iota((length, length), 1)).astype(F32)
    logs_t = -exact_dot(lower, decay, ((1,), (1,)))
    first = iota((heads, width), 0) * lanes
    channel = iota((heads, width), 1)
    spread = ((channel >= first) & (channel < first + lanes)).astype(F32)
    for load in loads[4:7]:
        load.wait()
    marks = jnp.broadcast_to(bound_ref[...].astype(F32), (slots, slots)).T
    marks = jnp.concatenate([marks] * (length // slots), axis=1)
    place = iota((slots, length), 1).astype(F32)
    hit = place == marks
    seen = place <= marks
    onehot = hit.astype(F32)
    c_rows = exact_dot(onehot, c_ref[...])
    logs_sel = exact_dot(onehot, logs_t)
    affinity = exact_dot(c_rows, b_ref[...], ((1,), (1,)))
    inside = []
    first_lane = iota((slots, pair_width), 1) < lanes
    for pair in range(pairs):
        both = x_both[pair]
        parts = []
        for h in (2 * pair, 2 * pair + 1):
            gap = logs_sel[:, h : h + 1] - logs[h : h + 1, :]
            weights = jnp.where(seen, jnp.exp(jnp.where(seen, gap, 0.0)), 0.0) * affinity
            weights = weights + jnp.where(hit, skip_ref[:, h : h + 1], 0.0)
            w_high, w_low = halves(weights)
            wide = fast_dot(w_high, both)
            parts.append(
                wide[:, :pair_width] + wide[:, pair_width:] + fast_dot(w_low, both[:, :pair_width])
            )
        inside.append(jnp.where(first_lane, parts[0], parts[1]))
    inside = jnp.concatenate(inside, axis=1)
    enter_scale = exact_dot(jnp.exp(logs_sel), spread)
    c_high, c_low = halves(c_rows)

    for d in range(1, seqs):
        source = shard_at(-d)
        tag_copy(shard_at(d), source, source).wait_recv()
    all_tags = tag_recv[...].reshape(seqs, state)
    tag_lane = iota((seqs, state), 1)

    def b_copy(s, j):
        return remote(send_b.at[s], recv_b.at[j], b_send.at[s], b_recv.at[j], (s, col))

    @pl.when(is_owner)
    def _():
        mine = me - lo
        even = jnp.sum(jnp.where(tag_lane == 2 * mine, all_tags, 0.0), axis=1, keepdims=True)
        odd = jnp.sum(jnp.where(tag_lane == 2 * mine + 1, all_tags, 0.0), axis=1, keepdims=True)
        kept = jnp.exp(jnp.where(iota((seqs, pair_width), 1) < lanes, even, odd))
        running = jnp.zeros((state, pair_width), F32)
        for s in range(seqs):
            send_b[s] = running.astype(BF16)

            @pl.when(me != s)
            def _():
                b_copy(s, mine).start()

            if s < seqs - 1:

                @pl.when(me != s)
                def _():
                    a_copy(mine, s).wait_recv()

                running = kept[s : s + 1] * running + recv_a[s].astype(F32)

        @pl.when(me != seqs - 1)
        def _():
            a_copy(mine, seqs - 1).wait_recv()

        recv_b[mine] = send_b[me]

    earlier = (iota((seqs, state), 0) < me) & (tag_lane == heads)
    start = jnp.sum(jnp.where(earlier, all_tags, 0.0), axis=(0, 1), keepdims=True)
    offset = start - (me * rows - half).astype(F32)
    slot = iota((slots, slots), 1).astype(F32)
    count = jnp.broadcast_to(counts_ref[...].astype(F32), (slots, slots))
    shift = (slot == iota((slots, slots), 0).astype(F32) - offset) & (slot < count)
    shift = shift.astype(BF16)

    for j in range(pairs):

        @pl.when(me != lo + j)
        def _():
            b_copy(me, j).wait_recv()

    entering = jnp.concatenate([recv_b[j] for j in range(pairs)], axis=1)
    carried = fast_dot(c_high, entering) + fast_dot(c_low, entering)
    y = (inside + enter_scale * carried).astype(BF16)
    window = fast_dot(shift, y).astype(BF16)
    loads[7].wait()
    partial = fast_dot(window, outw[...])
    pieces = slots // piece
    for i in range(pieces):
        send_p[i] = partial[i * piece : (i + 1) * piece, :].astype(BF16)
    outer = (pieces - groups) // 2

    def project(src, slot, k, peer):
        return remote(send_p.at[src], recv_p.at[slot], p_send.at[k], p_recv.at[slot], peer)

    below_sent = [project(i, groups + col, i, (shard_at(-1), groups - outer + i)) for i in range(outer)]
    above_sent = [
        project(outer + groups + i, groups + col, outer + i, (shard_at(1), i))
        for i in range(outer)
    ]
    sent = []
    for d in range(1, groups):
        to = head_at(d)
        sent.append(project(outer + to, col, 2 * outer + d - 1, (me, to)))
    has_below, has_above = me > 0, me < seqs - 1

    @pl.when(has_below)
    def _():
        for copy in below_sent:
            copy.start()

    @pl.when(has_above)
    def _():
        for copy in above_sent:
            copy.start()

    for copy in sent:
        copy.start()
    recv_p[col] = send_p[outer + col]
    expects = (has_below & (col < outer)) | (has_above & (col >= outer))

    @pl.when(expects)
    def _():
        for k in range(groups):
            project(0, groups + k, 0, (shard_at(1), k)).wait_recv()

    @pl.when(jnp.logical_not(expects))
    def _():
        recv_p[groups:] = jnp.zeros((groups, piece, recv_p.shape[2]), recv_p.dtype)

    for d in range(1, groups):
        source = head_at(groups - d)
        project(0, source, 0, (me, source)).wait_recv()
    loads[8].wait()
    mixed = recv_p[0].astype(F32)
    for k in range(1, 2 * groups):
        mixed = mixed + recv_p[k].astype(F32)
    square = jnp.mean(mixed * mixed, axis=-1, keepdims=True)
    normed = (mixed * lax.rsqrt(square + 1e-05) * gain_ref[...]).astype(BF16)
    recv_n[col] = normed

    def n_copy(to, source):
        return remote(recv_n.at[col], recv_n.at[source], n_sem.at[0, to], n_sem.at[1, source], (me, to))

    sent_n = [n_copy(to, col) for to in (other, other + 1, partner)]
    for copy in sent_n:
        copy.start()
    loads[9].wait()
    near = rows // CHUNKS
    quarter = near // 2
    left = iota((near, pair_width), 1) < lanes
    left_quarter = left[:quarter]

    def turned(a):
        return pltpu.roll(a, lanes, 1)

    def q_copy(to, slot, part):
        return remote(
            send_q.at[to, part],
            recv_q.at[slot, part],
            q_send.at[part, to],
            q_recv.at[part, slot],
            (to, col),
        )

    for sources, part in (((partner,), chip), ((other, other + 1), 1 - chip)):
        for source in sources:
            n_copy(source, source).wait_recv()
        block = recv_n[pl.ds(2 * part, 2)].reshape(near, -1)
        query, key, value = [
            fast_dot(block, qkvw[i]).astype(BF16).astype(F32) for i in range(3)
        ]
        for pair in range(pairs):
            at = slice(pair * pair_width, (pair + 1) * pair_width)
            q, k, v = query[:, at], key[:, at], value[:, at]
            above, below = v[:quarter], v[quarter:]
            send_q[2 * pair, part, :near, :] = jnp.where(left, q, turned(k)).astype(BF16)
            send_q[2 * pair + 1, part, :near, :] = jnp.where(left, turned(q), k).astype(BF16)
            send_q[2 * pair, part, near:, :] = jnp.where(left_quarter, above, turned(below)).astype(
                BF16
            )
            send_q[2 * pair + 1, part, near:, :] = jnp.where(
                left_quarter, turned(above), below
            ).astype(BF16)
        for to in targets:
            q_copy(to, me, part).start()
    recv_q[me] = send_q[me]

    def unpack(ref, at):
        both = ref[at, :, :near, :].reshape(rows, pair_width).astype(F32)
        packed = ref[at, :, near:, :].astype(F32)
        values = []
        for part in range(CHUNKS):
            values += [packed[part], turned(packed[part])]
        return both, values

    def attend(queries, keys, values, first_row):
        scores = fast_dot(queries, keys, ((1,), (1,))) * (lanes ** (-0.5))
        allowed = first_row + iota(scores.shape, 0) >= iota(scores.shape, 1)
        scores = jnp.where(allowed, scores, -1e30)
        highest = jnp.max(scores, axis=-1, keepdims=True)
        exps = jnp.where(allowed, jnp.exp(scores - highest), 0.0)
        total = jnp.sum(exps, axis=-1, keepdims=True)
        return fast_dot(exps.astype(BF16), values) / total

    @pl.when(me == 0)
    def _():
        left_rows = iota((rows, pair_width), 1) < lanes
        for pair in range(pairs):
            results = []
            for h in (2 * pair, 2 * pair + 1):
                both, values = unpack(send_q, h)
                queries = jnp.where(left_rows, both, 0.0).astype(BF16)
                keys = turned(both).astype(BF16)
                values = jnp.concatenate(values, axis=0).astype(BF16)
                results.append(attend(queries, keys, values, 0))
            out_ref[:, pair * pair_width : (pair + 1) * pair_width] = jnp.where(
                left_rows, results[0], turned(results[1])
            ).astype(out_ref.dtype)

    for part in (chip, 1 - chip):
        for d in range(1, seqs):
            source = shard_at(-d)
            q_copy(shard_at(d), source, part).wait_recv()
    wide, values = [], []
    for s in range(seqs):
        both, some = unpack(recv_q, s)
        wide.append(both)
        values += some
    wide = jnp.concatenate(wide, axis=0)
    values = jnp.concatenate(values, axis=0).astype(BF16)
    left_all = iota(wide.shape, 1) < lanes
    queries = jnp.where(left_all, wide, 0.0).astype(BF16)
    keys = turned(wide).astype(BF16)
    left_half = iota((half, pair_width), 1) < lanes

    def o_copy(s, slot):
        return remote(send_o.at[s], recv_o.at[slot], o_send.at[s], o_recv.at[slot], (s, col))

    span = 2 * rows
    for k in range(seqs // 2):
        end = (k + 1) * span
        result = attend(queries[k * span : end], keys[:end], values[:end], k * span)
        for s in (2 * k, 2 * k + 1):
            if s == 0:
                continue
            at = (s - 2 * k) * rows
            above, below = result[at : at + half], result[at + half : at + rows]
            send_o[s] = jnp.where(left_half, above, turned(below)).astype(BF16)

            @pl.when(me != s)
            def _():
                o_copy(s, me).start()

    @pl.when(me > 0)
    def _():
        recv_o[me] = send_o[me]
        for d in range(1, seqs):
            o_copy(me, shard_at(-d)).wait_recv()
        for pair in range(pairs):
            at = slice(pair * pair_width, (pair + 1) * pair_width)
            even, odd = recv_o[2 * pair].astype(F32), recv_o[2 * pair + 1].astype(F32)
            out_ref[:half, at] = jnp.where(left_half, even, turned(odd)).astype(out_ref.dtype)
            out_ref[half:, at] = jnp.where(left_half, turned(even), odd).astype(out_ref.dtype)

    for copy in sent + sent_n:
        copy.wait_send()

    @pl.when(has_below)
    def _():
        for copy in below_sent:
            copy.wait_send()

    @pl.when(has_above)
    def _():
        for copy in above_sent:
            copy.wait_send()

    for j in range(pairs):

        @pl.when(me != lo + j)
        def _():
            a_copy(j, me).wait_send()

    for to in targets:
        tag_copy(to, me, me).wait_send()
        for part in range(CHUNKS):
            q_copy(to, me, part).wait_send()

    for s in range(seqs):

        @pl.when(is_owner & (me != s))
        def _():
            b_copy(s, me - lo).wait_send()

        if s > 0:

            @pl.when(me != s)
            def _():
                o_copy(s, me).wait_send()


def fused_body(
    byte_input,
    b_proj,
    c_proj,
    step_decay,
    skip_gain,
    out_weight,
    boundaries,
    counts,
    norm_gain,
    qkv_weight,
):
    seqs, groups = lax.axis_size("seq"), lax.axis_size("head")
    heads = step_decay.shape[0]
    length, width = byte_input.shape
    lanes = width // heads
    pairs = heads // 2
    state = b_proj.shape[1]
    rows = ROWS_DEV
    piece = rows // groups
    enc = out_weight.shape[1]
    pieces = boundaries.shape[1] // piece
    packed = rows // CHUNKS + rows // (2 * CHUNKS)
    vmem = pl.BlockSpec(memory_space=pltpu.VMEM)
    hbm = pl.BlockSpec(memory_space=pl.ANY)
    dma = pltpu.SemaphoreType.DMA
    operands = (
        step_decay,
        byte_input,
        b_proj,
        counts.reshape(1, 1),
        boundaries,
        c_proj,
        skip_gain.reshape(1, -1),
        out_weight,
        norm_gain.reshape(1, -1),
        qkv_weight,
    )
    result = pl.pallas_call(
        functools.partial(fused, seqs, groups),
        out_shape=jax.ShapeDtypeStruct((rows, width), BF16),
        in_specs=[hbm] * len(operands),
        out_specs=vmem,
        scratch_shapes=[pltpu.VMEM(array.shape, array.dtype) for array in operands]
        + [
            pltpu.VMEM((pairs, length, 4 * lanes), BF16),
            pltpu.VMEM((1, state), F32),
            pltpu.VMEM((seqs, 1, state), F32),
            pltpu.VMEM((pairs, state, 2 * lanes), BF16),
            pltpu.VMEM((seqs, state, 2 * lanes), BF16),
            pltpu.VMEM((seqs, state, 2 * lanes), BF16),
            pltpu.VMEM((pairs, state, 2 * lanes), BF16),
            pltpu.VMEM((pieces, piece, enc), BF16),
            pltpu.VMEM((2 * groups, piece, enc), BF16),
            pltpu.VMEM((groups, piece, enc), BF16),
            pltpu.VMEM((seqs, CHUNKS, packed, 2 * lanes), BF16),
            pltpu.VMEM((seqs, CHUNKS, packed, 2 * lanes), BF16),
            pltpu.VMEM((seqs, rows // 2, 2 * lanes), BF16),
            pltpu.VMEM((seqs, rows // 2, 2 * lanes), BF16),
            dma((len(operands),)),
            dma((2, seqs)),
            dma((pairs,)),
            dma((seqs,)),
            dma((seqs,)),
            dma((pairs,)),
            dma((2 * groups,)),
            dma((2 * groups,)),
            dma((2, groups)),
            dma((CHUNKS, seqs)),
            dma((CHUNKS, seqs)),
            dma((seqs,)),
            dma((seqs,)),
        ],
        compiler_params=pltpu.CompilerParams(collective_id=0, has_side_effects=True),
    )(*operands)
    return result.astype(F32)


def chosen(*args):
    byte_input, step_decay, slots = args[0], args[3], args[6].shape[1]
    heads = step_decay.shape[0]
    lanes = byte_input.shape[1] // heads
    seqs, groups = lax.axis_size("seq"), lax.axis_size("head")
    fits = seqs == heads and lanes == ATT_DIM and args[9].shape[2] == byte_input.shape[1]
    fits = fits and 2 * lanes == slots and args[1].shape[1] == slots and slots == 2 * ROWS_DEV
    fits = fits and seqs % 4 == 0 and groups == 2 * CHUNKS and ROWS_DEV % (16 * groups) == 0
    fits = fits and byte_input.shape[0] % slots == 0
    return fused_body(*args) if fits else body(*args)


def solution(mesh):
    return jax.shard_map(
        chosen,
        mesh=mesh,
        in_specs=(
            P("seq", "head"),
            P("seq", None),
            P("seq", None),
            P("head", "seq"),
            P("head"),
            P("head", None),
            P("seq", None),
            P("seq"),
            P(),
            P(None, None, "head"),
        ),
        out_specs=P("seq", "head"),
        check_vma=False,
    )
```

```python
import functools

import jax
import jax.numpy as jnp
from jax import lax
from jax.experimental import pallas as pl
from jax.experimental.pallas import tpu as pltpu
from jax.sharding import PartitionSpec as P

ATT_DIM = 64
ROWS_DEV = 64


def prefix(shard, axis, combine, identity):
    length, here = (lax.axis_size(axis), lax.axis_index(axis))
    everything = jax.tree.map(lambda part: lax.all_gather(part, axis), shard)
    start = jax.tree.map(
        lambda part, zero: jnp.broadcast_to(jnp.asarray(zero, part.dtype), part.shape),
        shard,
        identity,
    )

    def lap(k, before):
        reached = k < here
        new = combine(before, jax.tree.map(lambda part: part[k], everything))
        return jax.tree.map(lambda a, b: jnp.where(reached, a, b), new, before)

    return lax.fori_loop(0, length, lap, start)


def extended(cells, sides, width):
    for axis, dim in sides:
        count = lax.axis_size(axis)
        ends = count - 1
        head = lax.slice_in_dim(cells, 0, width, axis=dim)
        tail = lax.slice_in_dim(cells, cells.shape[dim] - width, cells.shape[dim], axis=dim)
        cells = jnp.concatenate(
            [
                lax.ppermute(tail, axis, [(i, (i + 1) % count) for i in range(ends)]),
                cells,
                lax.ppermute(head, axis, [((i + 1) % count, i) for i in range(ends)]),
            ],
            axis=dim,
        )
    return cells


def state_space(inputs, b_rows, c_rows, decay):
    log_decay = jnp.cumsum(-decay, axis=1)
    affinity = jnp.dot(c_rows, b_rows.T, precision=lax.Precision.HIGHEST)
    length = inputs.shape[0]
    causal = lax.broadcasted_iota(jnp.int32, (length, length), 0) >= lax.broadcasted_iota(
        jnp.int32, (length, length), 1
    )

    def one_head(pair):
        values, logs = pair
        weights = (
            jnp.where(causal, jnp.exp(jnp.where(causal, logs[:, None] - logs[None, :], 0.0)), 0.0)
            * affinity
        )
        return jnp.dot(weights, values, precision=lax.Precision.HIGHEST)

    inside = lax.map(one_head, (inputs.transpose(1, 0, 2), log_decay))
    tail = jnp.exp(log_decay[:, -1:] - log_decay)
    own_state = jnp.einsum("ht,thp,tn->hpn", tail, inputs, b_rows, precision=lax.Precision.HIGHEST)
    return (log_decay, inside, own_state)


def link(earlier, later):
    return (earlier[0] * later[0], later[0][:, None, None] * earlier[1] + later[1])


def body(
    byte_input,
    b_proj,
    c_proj,
    step_decay,
    skip_gain,
    out_weight,
    boundaries,
    counts,
    norm_gain,
    qkv_weight,
):
    heads_here = step_decay.shape[0]
    length = byte_input.shape[0]
    inputs = byte_input.reshape(length, heads_here, -1)
    log_decay, inside, own_state = state_space(inputs, b_proj, c_proj, step_decay)
    span_decay = jnp.exp(log_decay[:, -1])
    arriving = prefix(
        (span_decay, own_state), "seq", link, (jnp.ones_like(span_decay), jnp.zeros_like(own_state))
    )
    carried = jnp.exp(log_decay)[:, :, None] * jnp.einsum(
        "tn,hpn->htp", c_proj, arriving[1], precision=lax.Precision.HIGHEST
    )
    mixed_heads = inside + carried + skip_gain[:, None, None] * inputs.transpose(1, 0, 2)
    slots = boundaries.shape[1]
    picked = jnp.take(mixed_heads, boundaries[0], axis=1)
    selected = picked.transpose(1, 0, 2).reshape(slots, -1).astype(jnp.bfloat16)
    all_counts = lax.all_gather(counts, "seq", axis=0, tiled=True)
    starts = jnp.cumsum(all_counts) - all_counts
    myself = lax.axis_index("seq")
    shards = lax.axis_size("seq")
    slot = jnp.arange(slots, dtype=jnp.int32)

    def slot_index(source):
        inside_axis = (source >= 0) & (source < shards)
        safe = jnp.clip(source, 0, shards - 1)
        begin = jnp.take(starts, safe)
        number = jnp.take(all_counts, safe)
        return jnp.where(inside_axis & (slot < number), begin + slot, -1)

    global_index = jnp.concatenate(
        [slot_index(myself - 1), slot_index(myself), slot_index(myself + 1)]
    )
    first_row = myself * ROWS_DEV
    target = first_row + jnp.arange(ROWS_DEV, dtype=jnp.int32)
    picker = global_index[None, :] == target[:, None]
    nearby = extended(selected, (("seq", 0),), slots)
    owned = jnp.dot(picker.astype(jnp.bfloat16), nearby, preferred_element_type=jnp.float32).astype(
        jnp.bfloat16
    )
    partial_value = jnp.dot(owned, out_weight, preferred_element_type=jnp.float32)
    packed = lax.psum(partial_value, "head")
    normed = (
        packed * lax.rsqrt(jnp.mean(packed * packed, axis=-1, keepdims=True) + 1e-05) * norm_gain
    ).astype(jnp.bfloat16)
    query = jnp.dot(normed, qkv_weight[0], preferred_element_type=jnp.float32).astype(jnp.bfloat16)
    keyed = jnp.dot(normed, qkv_weight[1], preferred_element_type=jnp.float32).astype(jnp.bfloat16)
    valued = jnp.dot(normed, qkv_weight[2], preferred_element_type=jnp.float32).astype(jnp.bfloat16)
    att_here = query.shape[1] // ATT_DIM
    queries = query.reshape(ROWS_DEV, att_here, ATT_DIM)
    row_place = first_row + jnp.arange(ROWS_DEV, dtype=jnp.int32)
    scale = ATT_DIM ** (-0.5)
    running = jnp.full((att_here, ROWS_DEV), -1e30, jnp.float32)
    key_piece = lax.all_gather(keyed, "seq", axis=0, tiled=True)
    value_piece = lax.all_gather(valued, "seq", axis=0, tiled=True)
    count = key_piece.shape[0]
    key_heads = key_piece.reshape(count, att_here, ATT_DIM)
    value_heads = value_piece.reshape(count, att_here, ATT_DIM)
    scores = (
        jnp.einsum("qhd,khd->hqk", queries, key_heads, preferred_element_type=jnp.float32) * scale
    )
    allowed = jnp.arange(count, dtype=jnp.int32)[None, :] <= row_place[:, None]
    scores = jnp.where(allowed[None], scores, -1e30)
    highest = jnp.maximum(running, jnp.max(scores, axis=-1))
    exps = jnp.where(allowed[None], jnp.exp(scores - highest[:, :, None]), 0.0)
    totals = jnp.sum(exps, axis=-1)
    weights = exps.astype(jnp.bfloat16)
    accum = jnp.einsum("hqk,khd->hqd", weights, value_heads, preferred_element_type=jnp.float32)
    running, totals, accum = (highest, totals, accum)
    result = accum / totals[:, :, None]
    return result.transpose(1, 0, 2).reshape(ROWS_DEV, att_here * ATT_DIM)


F32 = jnp.float32
BF16 = jnp.bfloat16
CHUNKS = 2


def exact_dot(a, b, dims=((1,), (0,))):
    return lax.dot_general(
        a, b, (dims, ((), ())), precision=lax.Precision.HIGHEST, preferred_element_type=F32
    )


def fast_dot(a, b, dims=((1,), (0,))):
    return lax.dot_general(a, b, (dims, ((), ())), preferred_element_type=F32)


def halves(a):
    high = a.astype(BF16)
    return high, (a - high.astype(F32)).astype(BF16)


def iota(shape, dim):
    return lax.broadcasted_iota(jnp.int32, shape, dim)


def fused(
    seqs,
    groups,
    decay_hbm,
    x_hbm,
    b_hbm,
    counts_hbm,
    bound_hbm,
    c_hbm,
    skip_hbm,
    outw_hbm,
    gain_hbm,
    qkvw_hbm,
    out_ref,
    decay_ref,
    x_ref,
    b_ref,
    counts_ref,
    bound_ref,
    c_ref,
    skip_ref,
    outw,
    gain_ref,
    qkvw,
    x_both,
    tag_send,
    tag_recv,
    send_a,
    recv_a,
    send_b,
    recv_b,
    send_p,
    recv_p,
    recv_n,
    send_q,
    recv_q,
    send_o,
    first_out,
    weight_sem,
    tag_sem,
    a_send,
    a_recv,
    b_send,
    b_recv,
    p_send,
    p_recv,
    n_sem,
    q_send,
    q_recv,
    o_send,
    o_recv,
    out_sem,
):
    me = lax.axis_index("seq")
    col = lax.axis_index("head")
    length, width = x_ref.shape
    heads = decay_ref.shape[0]
    lanes = width // heads
    pair_width = 2 * lanes
    pairs = heads // 2
    state = b_ref.shape[1]
    slots = bound_ref.shape[1]
    rows = out_ref.shape[0]
    piece = rows // groups
    half = rows // 2
    lo = (seqs - pairs) // 2
    is_owner = (me >= lo) & (me < lo + pairs)

    def shard_at(d):
        return lax.rem(me + d + seqs, seqs)

    layers = seqs // 2
    mid = layers // 2
    layer, side = me // 2, lax.rem(me, 2)
    near_end = layer < mid
    far_layers = [jnp.where(near_end, layers - 1 - k, k) for k in range(layers - mid)]
    same = jnp.where(near_end, layer, layer - (layers - mid))
    for k in range(1, mid):
        turn = lax.rem(same + k, mid)
        far_layers.append(jnp.where(near_end, turn, turn + (layers - mid)))
    targets = []
    for there in far_layers + [layer]:
        targets.append(2 * there + 1 - side)
        if there is not layer:
            targets.append(2 * there + side)

    def head_at(d):
        return lax.rem(col + d, groups)

    chip = col // 2
    partner = 2 * chip + 1 - lax.rem(col, 2)
    other = 2 * (1 - chip)

    barrier = pltpu.get_barrier_semaphore()
    peers = [(shard_at(d), col) for d in range(1, seqs)]
    peers += [(me, head_at(d)) for d in range(1, groups)]
    peers += [(shard_at(e), head_at(d)) for e in (-1, 1) for d in range(1, groups)]
    for peer in peers:
        pl.semaphore_signal(
            barrier, inc=1, device_id=peer, device_id_type=pl.DeviceIdType.MESH
        )

    def remote(src, dst, send_sem, recv_sem, peer):
        return pltpu.make_async_remote_copy(
            src_ref=src,
            dst_ref=dst,
            send_sem=send_sem,
            recv_sem=recv_sem,
            device_id=peer,
            device_id_type=pl.DeviceIdType.MESH,
        )

    loads = [
        pltpu.make_async_copy(source, target, weight_sem.at[i])
        for i, (source, target) in enumerate(
            (
                (decay_hbm, decay_ref),
                (x_hbm, x_ref),
                (b_hbm, b_ref),
                (counts_hbm, counts_ref),
                (bound_hbm, bound_ref),
                (c_hbm, c_ref),
                (skip_hbm, skip_ref),
                (outw_hbm, outw),
                (gain_hbm, gain_ref),
                (qkvw_hbm, qkvw),
            )
        )
    ]
    for load in loads[:7]:
        load.start()

    loads[0].wait()
    decay = decay_ref[...]
    upper = (iota((length, length), 0) <= iota((length, length), 1)).astype(F32)
    logs = -exact_dot(decay, upper)
    tail = jnp.exp(logs[:, length - 1 : length] - logs)
    loads[3].wait()
    tag_row = iota((heads, state), 1) == iota((heads, state), 0)
    tags = jnp.where(tag_row, logs[:, length - 1 : length], 0.0)
    tags = jnp.sum(tags, axis=0, keepdims=True)
    number = jnp.broadcast_to(counts_ref[...].astype(F32), (1, state))
    tag_send[...] = jnp.where(iota((1, state), 1) == heads, number, tags)
    loads[1].wait()
    loads[2].wait()
    for load in loads[7:]:
        load.start()
    b_turned = b_ref[...].T
    first_half = iota((state, pair_width), 1) < lanes
    for pair in range(pairs):
        x_high, x_low = halves(x_ref[:, pair * pair_width : (pair + 1) * pair_width])
        both = jnp.concatenate([x_high, x_low], axis=1)
        x_both[pair] = both
        faded = [b_turned * tail[h : h + 1, :] for h in (2 * pair, 2 * pair + 1)]
        f_high, f_low = halves(jnp.concatenate(faded, axis=0))
        wide = fast_dot(f_high, both)
        own = wide[:, :pair_width] + wide[:, pair_width:] + fast_dot(f_low, x_high)
        send_a[pair] = jnp.where(first_half, own[:state], own[state:]).astype(BF16)
    pl.semaphore_wait(barrier, len(peers))

    def tag_copy(to, slot, source):
        return remote(tag_send, tag_recv.at[slot], tag_sem.at[0, to], tag_sem.at[1, source], (to, col))

    def a_copy(j, slot):
        return remote(send_a.at[j], recv_a.at[slot], a_send.at[j], a_recv.at[slot], (lo + j, col))

    for to in targets:
        tag_copy(to, me, me).start()
    for k in range(pairs):
        j = jnp.where(near_end, pairs - 1 - k, k)

        @pl.when(me != lo + j)
        def _():
            a_copy(j, me).start()

    tag_recv[me] = tag_send[...]

    @pl.when(is_owner)
    def _():
        recv_a[me] = send_a[me - lo]

    lower = (iota((length, length), 0) >= iota((length, length), 1)).astype(F32)
    logs_t = -exact_dot(lower, decay, ((1,), (1,)))
    first = iota((heads, width), 0) * lanes
    channel = iota((heads, width), 1)
    spread = ((channel >= first) & (channel < first + lanes)).astype(F32)
    for load in loads[4:7]:
        load.wait()
    marks = jnp.broadcast_to(bound_ref[...].astype(F32), (slots, slots)).T
    marks = jnp.concatenate([marks] * (length // slots), axis=1)
    place = iota((slots, length), 1).astype(F32)
    hit = place == marks
    seen = place <= marks
    onehot = hit.astype(F32)
    c_rows = exact_dot(onehot, c_ref[...])
    logs_sel = exact_dot(onehot, logs_t)
    affinity = exact_dot(c_rows, b_ref[...], ((1,), (1,)))
    inside = []
    first_lane = iota((slots, pair_width), 1) < lanes
    for pair in range(pairs):
        both = x_both[pair]
        parts = []
        for h in (2 * pair, 2 * pair + 1):
            gap = logs_sel[:, h : h + 1] - logs[h : h + 1, :]
            weights = jnp.where(seen, jnp.exp(jnp.where(seen, gap, 0.0)), 0.0) * affinity
            weights = weights + jnp.where(hit, skip_ref[:, h : h + 1], 0.0)
            w_high, w_low = halves(weights)
            wide = fast_dot(w_high, both)
            parts.append(
                wide[:, :pair_width] + wide[:, pair_width:] + fast_dot(w_low, both[:, :pair_width])
            )
        inside.append(jnp.where(first_lane, parts[0], parts[1]))
    inside = jnp.concatenate(inside, axis=1)
    enter_scale = exact_dot(jnp.exp(logs_sel), spread)
    c_high, c_low = halves(c_rows)

    for d in range(1, seqs):
        source = shard_at(-d)
        tag_copy(shard_at(d), source, source).wait_recv()
    all_tags = tag_recv[...].reshape(seqs, state)
    tag_lane = iota((seqs, state), 1)

    def b_copy(s, j):
        return remote(send_b.at[s], recv_b.at[j], b_send.at[s], b_recv.at[j], (s, col))

    @pl.when(is_owner)
    def _():
        mine = me - lo
        even = jnp.sum(jnp.where(tag_lane == 2 * mine, all_tags, 0.0), axis=1, keepdims=True)
        odd = jnp.sum(jnp.where(tag_lane == 2 * mine + 1, all_tags, 0.0), axis=1, keepdims=True)
        kept = jnp.exp(jnp.where(iota((seqs, pair_width), 1) < lanes, even, odd))
        running = jnp.zeros((state, pair_width), F32)
        for s in range(seqs):
            send_b[s] = running.astype(BF16)

            @pl.when(me != s)
            def _():
                b_copy(s, mine).start()

            if s < seqs - 1:

                @pl.when(me != s)
                def _():
                    a_copy(mine, s).wait_recv()

                running = kept[s : s + 1] * running + recv_a[s].astype(F32)

        @pl.when(me != seqs - 1)
        def _():
            a_copy(mine, seqs - 1).wait_recv()

        recv_b[mine] = send_b[me]

    earlier = (iota((seqs, state), 0) < me) & (tag_lane == heads)
    start = jnp.sum(jnp.where(earlier, all_tags, 0.0), axis=(0, 1), keepdims=True)
    offset = start - (me * rows - half).astype(F32)
    slot = iota((slots, slots), 1).astype(F32)
    count = jnp.broadcast_to(counts_ref[...].astype(F32), (slots, slots))
    shift = (slot == iota((slots, slots), 0).astype(F32) - offset) & (slot < count)
    shift = shift.astype(BF16)

    for j in range(pairs):

        @pl.when(me != lo + j)
        def _():
            b_copy(me, j).wait_recv()

    entering = jnp.concatenate([recv_b[j] for j in range(pairs)], axis=1)
    carried = fast_dot(c_high, entering) + fast_dot(c_low, entering)
    y = (inside + enter_scale * carried).astype(BF16)
    window = fast_dot(shift, y).astype(BF16)
    loads[7].wait()
    partial = fast_dot(window, outw[...])
    pieces = slots // piece
    for i in range(pieces):
        send_p[i] = partial[i * piece : (i + 1) * piece, :].astype(BF16)
    outer = (pieces - groups) // 2

    def project(src, slot, k, peer):
        return remote(send_p.at[src], recv_p.at[slot], p_send.at[k], p_recv.at[slot], peer)

    below_sent = [project(i, groups + col, i, (shard_at(-1), groups - outer + i)) for i in range(outer)]
    above_sent = [
        project(outer + groups + i, groups + col, outer + i, (shard_at(1), i))
        for i in range(outer)
    ]
    sent = []
    for d in range(1, groups):
        to = head_at(d)
        sent.append(project(outer + to, col, 2 * outer + d - 1, (me, to)))
    has_below, has_above = me > 0, me < seqs - 1

    @pl.when(has_below)
    def _():
        for copy in below_sent:
            copy.start()

    @pl.when(has_above)
    def _():
        for copy in above_sent:
            copy.start()

    for copy in sent:
        copy.start()
    recv_p[col] = send_p[outer + col]
    expects = (has_below & (col < outer)) | (has_above & (col >= outer))

    @pl.when(expects)
    def _():
        for k in range(groups):
            project(0, groups + k, 0, (shard_at(1), k)).wait_recv()

    @pl.when(jnp.logical_not(expects))
    def _():
        recv_p[groups:] = jnp.zeros((groups, piece, recv_p.shape[2]), recv_p.dtype)

    for d in range(1, groups):
        source = head_at(groups - d)
        project(0, source, 0, (me, source)).wait_recv()
    loads[8].wait()
    mixed = recv_p[0].astype(F32)
    for k in range(1, 2 * groups):
        mixed = mixed + recv_p[k].astype(F32)
    square = jnp.mean(mixed * mixed, axis=-1, keepdims=True)
    normed = (mixed * lax.rsqrt(square + 1e-05) * gain_ref[...]).astype(BF16)
    recv_n[col] = normed

    def n_copy(to, source):
        return remote(recv_n.at[col], recv_n.at[source], n_sem.at[0, to], n_sem.at[1, source], (me, to))

    sent_n = [n_copy(to, col) for to in (other, other + 1, partner)]
    for copy in sent_n:
        copy.start()
    loads[9].wait()
    near = rows // CHUNKS

    def q_copy(j, slot, part):
        return remote(
            send_q.at[j, part],
            recv_q.at[slot, part],
            q_send.at[part, j],
            q_recv.at[part, slot],
            (lo + j, col),
        )

    for sources, part in (((partner,), chip), ((other, other + 1), 1 - chip)):
        for source in sources:
            n_copy(source, source).wait_recv()
        block = recv_n[pl.ds(2 * part, 2)].reshape(near, -1)
        for i in range(3):
            product = fast_dot(block, qkvw[i]).astype(BF16)
            for pair in range(pairs):
                send_q[pair, part, i] = product[:, pair * pair_width : (pair + 1) * pair_width]
        for k in range(pairs):
            j = jnp.where(near_end, pairs - 1 - k, k)

            @pl.when(me != lo + j)
            def _():
                q_copy(j, me, part).start()

    def attend(queries, keys, values, first_row):
        left = iota(queries.shape, 1) < lanes
        results = []
        for keep in (left, jnp.logical_not(left)):
            masked = jnp.where(keep, queries.astype(F32), 0.0).astype(BF16)
            scores = fast_dot(masked, keys, ((1,), (1,))) * (lanes ** (-0.5))
            allowed = first_row + iota(scores.shape, 0) >= iota(scores.shape, 1)
            scores = jnp.where(allowed, scores, -1e30)
            highest = jnp.max(scores, axis=-1, keepdims=True)
            exps = jnp.where(allowed, jnp.exp(scores - highest), 0.0)
            total = jnp.sum(exps, axis=-1, keepdims=True)
            results.append(fast_dot(exps.astype(BF16), values) / total)
        return jnp.where(left, results[0], results[1]).astype(BF16)

    @pl.when(me == 0)
    def _():
        for pair in range(pairs):
            q, k, v = [send_q[pair, :, i].reshape(rows, pair_width) for i in range(3)]
            first_out[:, pair * pair_width : (pair + 1) * pair_width] = attend(q, k, v, 0)
        pltpu.make_async_copy(first_out, out_ref, out_sem).start()

    def o_copy(s, j):
        place = pl.ds(pl.multiple_of(j * pair_width, pair_width), pair_width)
        return remote(send_o.at[s], out_ref.at[:, place], o_send.at[s], o_recv.at[j], (s, col))

    def o_keep(j):
        place = pl.ds(pl.multiple_of(j * pair_width, pair_width), pair_width)
        return pltpu.make_async_copy(send_o.at[me], out_ref.at[:, place], out_sem)

    @pl.when(is_owner)
    def _():
        mine = me - lo
        recv_q[me] = send_q[mine]
        for part in (chip, 1 - chip):
            for d in range(1, seqs):
                q_copy(mine, shard_at(-d), part).wait_recv()
        q, k, v = [recv_q[:, :, i].reshape(seqs * rows, pair_width) for i in range(3)]
        span = 2 * rows
        for n in range(seqs // 2):
            end = (n + 1) * span
            result = attend(q[n * span : end], k[:end], v[:end], n * span)
            for s in (2 * n, 2 * n + 1):
                if s == 0:
                    continue
                send_o[s] = result[(s - 2 * n) * rows : (s - 2 * n + 1) * rows]

                @pl.when(me != s)
                def _():
                    o_copy(s, mine).start()

        o_keep(mine).start()
        o_keep(mine).wait()

    @pl.when(me == 0)
    def _():
        pltpu.make_async_copy(first_out, out_ref, out_sem).wait()

    for j in range(pairs):

        @pl.when((me > 0) & (me != lo + j))
        def _():
            o_copy(me, j).wait_recv()

    for copy in sent + sent_n:
        copy.wait_send()

    @pl.when(has_below)
    def _():
        for copy in below_sent:
            copy.wait_send()

    @pl.when(has_above)
    def _():
        for copy in above_sent:
            copy.wait_send()

    for j in range(pairs):

        @pl.when(me != lo + j)
        def _():
            a_copy(j, me).wait_send()
            for part in range(CHUNKS):
                q_copy(j, me, part).wait_send()

    for to in targets:
        tag_copy(to, me, me).wait_send()

    for s in range(seqs):

        @pl.when(is_owner & (me != s))
        def _():
            b_copy(s, me - lo).wait_send()

        if s > 0:

            @pl.when(is_owner & (me != s))
            def _():
                o_copy(s, me - lo).wait_send()


def fused_body(
    byte_input,
    b_proj,
    c_proj,
    step_decay,
    skip_gain,
    out_weight,
    boundaries,
    counts,
    norm_gain,
    qkv_weight,
):
    seqs, groups = lax.axis_size("seq"), lax.axis_size("head")
    heads = step_decay.shape[0]
    length, width = byte_input.shape
    lanes = width // heads
    pairs = heads // 2
    state = b_proj.shape[1]
    rows = ROWS_DEV
    piece = rows // groups
    enc = out_weight.shape[1]
    pieces = boundaries.shape[1] // piece
    hbm = pl.BlockSpec(memory_space=pl.ANY)
    dma = pltpu.SemaphoreType.DMA
    operands = (
        step_decay,
        byte_input,
        b_proj,
        counts.reshape(1, 1),
        boundaries,
        c_proj,
        skip_gain.reshape(1, -1),
        out_weight,
        norm_gain.reshape(1, -1),
        qkv_weight,
    )
    result = pl.pallas_call(
        functools.partial(fused, seqs, groups),
        out_shape=jax.ShapeDtypeStruct((rows, width), BF16),
        in_specs=[hbm] * len(operands),
        out_specs=hbm,
        scratch_shapes=[pltpu.VMEM(array.shape, array.dtype) for array in operands]
        + [
            pltpu.VMEM((pairs, length, 4 * lanes), BF16),
            pltpu.VMEM((1, state), F32),
            pltpu.VMEM((seqs, 1, state), F32),
            pltpu.VMEM((pairs, state, 2 * lanes), BF16),
            pltpu.VMEM((seqs, state, 2 * lanes), BF16),
            pltpu.VMEM((seqs, state, 2 * lanes), BF16),
            pltpu.VMEM((pairs, state, 2 * lanes), BF16),
            pltpu.VMEM((pieces, piece, enc), BF16),
            pltpu.VMEM((2 * groups, piece, enc), BF16),
            pltpu.VMEM((groups, piece, enc), BF16),
            pltpu.VMEM((pairs, CHUNKS, 3, rows // CHUNKS, 2 * lanes), BF16),
            pltpu.VMEM((seqs, CHUNKS, 3, rows // CHUNKS, 2 * lanes), BF16),
            pltpu.VMEM((seqs, rows, 2 * lanes), BF16),
            pltpu.VMEM((rows, width), BF16),
            dma((len(operands),)),
            dma((2, seqs)),
            dma((pairs,)),
            dma((seqs,)),
            dma((seqs,)),
            dma((pairs,)),
            dma((2 * groups,)),
            dma((2 * groups,)),
            dma((2, groups)),
            dma((CHUNKS, pairs)),
            dma((CHUNKS, seqs)),
            dma((seqs,)),
            dma((pairs,)),
            dma,
        ],
        compiler_params=pltpu.CompilerParams(collective_id=0, has_side_effects=True),
    )(*operands)
    return result.astype(F32)


def chosen(*args):
    byte_input, step_decay, slots = args[0], args[3], args[6].shape[1]
    heads = step_decay.shape[0]
    lanes = byte_input.shape[1] // heads
    seqs, groups = lax.axis_size("seq"), lax.axis_size("head")
    fits = seqs == heads and lanes == ATT_DIM and args[9].shape[2] == byte_input.shape[1]
    fits = fits and 2 * lanes == slots and args[1].shape[1] == slots and slots == 2 * ROWS_DEV
    fits = fits and seqs % 4 == 0 and groups == 2 * CHUNKS and ROWS_DEV % (16 * groups) == 0
    fits = fits and byte_input.shape[0] % slots == 0
    return fused_body(*args) if fits else body(*args)


def solution(mesh):
    return jax.shard_map(
        chosen,
        mesh=mesh,
        in_specs=(
            P("seq", "head"),
            P("seq", None),
            P("seq", None),
            P("head", "seq"),
            P("head"),
            P("head", None),
            P("seq", None),
            P("seq"),
            P(),
            P(None, None, "head"),
        ),
        out_specs=P("seq", "head"),
        check_vma=False,
    )
```

```python
import functools

import jax
import jax.numpy as jnp
from jax import lax
from jax.experimental import pallas as pl
from jax.experimental.pallas import tpu as pltpu
from jax.sharding import PartitionSpec as P

ATT_DIM = 64
ROWS_DEV = 64


def prefix(shard, axis, combine, identity):
    length, here = (lax.axis_size(axis), lax.axis_index(axis))
    everything = jax.tree.map(lambda part: lax.all_gather(part, axis), shard)
    start = jax.tree.map(
        lambda part, zero: jnp.broadcast_to(jnp.asarray(zero, part.dtype), part.shape),
        shard,
        identity,
    )

    def lap(k, before):
        reached = k < here
        new = combine(before, jax.tree.map(lambda part: part[k], everything))
        return jax.tree.map(lambda a, b: jnp.where(reached, a, b), new, before)

    return lax.fori_loop(0, length, lap, start)


def extended(cells, sides, width):
    for axis, dim in sides:
        count = lax.axis_size(axis)
        ends = count - 1
        head = lax.slice_in_dim(cells, 0, width, axis=dim)
        tail = lax.slice_in_dim(cells, cells.shape[dim] - width, cells.shape[dim], axis=dim)
        cells = jnp.concatenate(
            [
                lax.ppermute(tail, axis, [(i, (i + 1) % count) for i in range(ends)]),
                cells,
                lax.ppermute(head, axis, [((i + 1) % count, i) for i in range(ends)]),
            ],
            axis=dim,
        )
    return cells


def state_space(inputs, b_rows, c_rows, decay):
    log_decay = jnp.cumsum(-decay, axis=1)
    affinity = jnp.dot(c_rows, b_rows.T, precision=lax.Precision.HIGHEST)
    length = inputs.shape[0]
    causal = lax.broadcasted_iota(jnp.int32, (length, length), 0) >= lax.broadcasted_iota(
        jnp.int32, (length, length), 1
    )

    def one_head(pair):
        values, logs = pair
        weights = (
            jnp.where(causal, jnp.exp(jnp.where(causal, logs[:, None] - logs[None, :], 0.0)), 0.0)
            * affinity
        )
        return jnp.dot(weights, values, precision=lax.Precision.HIGHEST)

    inside = lax.map(one_head, (inputs.transpose(1, 0, 2), log_decay))
    tail = jnp.exp(log_decay[:, -1:] - log_decay)
    own_state = jnp.einsum("ht,thp,tn->hpn", tail, inputs, b_rows, precision=lax.Precision.HIGHEST)
    return (log_decay, inside, own_state)


def link(earlier, later):
    return (earlier[0] * later[0], later[0][:, None, None] * earlier[1] + later[1])


def body(
    byte_input,
    b_proj,
    c_proj,
    step_decay,
    skip_gain,
    out_weight,
    boundaries,
    counts,
    norm_gain,
    qkv_weight,
):
    heads_here = step_decay.shape[0]
    length = byte_input.shape[0]
    inputs = byte_input.reshape(length, heads_here, -1)
    log_decay, inside, own_state = state_space(inputs, b_proj, c_proj, step_decay)
    span_decay = jnp.exp(log_decay[:, -1])
    arriving = prefix(
        (span_decay, own_state), "seq", link, (jnp.ones_like(span_decay), jnp.zeros_like(own_state))
    )
    carried = jnp.exp(log_decay)[:, :, None] * jnp.einsum(
        "tn,hpn->htp", c_proj, arriving[1], precision=lax.Precision.HIGHEST
    )
    mixed_heads = inside + carried + skip_gain[:, None, None] * inputs.transpose(1, 0, 2)
    slots = boundaries.shape[1]
    picked = jnp.take(mixed_heads, boundaries[0], axis=1)
    selected = picked.transpose(1, 0, 2).reshape(slots, -1).astype(jnp.bfloat16)
    all_counts = lax.all_gather(counts, "seq", axis=0, tiled=True)
    starts = jnp.cumsum(all_counts) - all_counts
    myself = lax.axis_index("seq")
    shards = lax.axis_size("seq")
    slot = jnp.arange(slots, dtype=jnp.int32)

    def slot_index(source):
        inside_axis = (source >= 0) & (source < shards)
        safe = jnp.clip(source, 0, shards - 1)
        begin = jnp.take(starts, safe)
        number = jnp.take(all_counts, safe)
        return jnp.where(inside_axis & (slot < number), begin + slot, -1)

    global_index = jnp.concatenate(
        [slot_index(myself - 1), slot_index(myself), slot_index(myself + 1)]
    )
    first_row = myself * ROWS_DEV
    target = first_row + jnp.arange(ROWS_DEV, dtype=jnp.int32)
    picker = global_index[None, :] == target[:, None]
    nearby = extended(selected, (("seq", 0),), slots)
    owned = jnp.dot(picker.astype(jnp.bfloat16), nearby, preferred_element_type=jnp.float32).astype(
        jnp.bfloat16
    )
    partial_value = jnp.dot(owned, out_weight, preferred_element_type=jnp.float32)
    packed = lax.psum(partial_value, "head")
    normed = (
        packed * lax.rsqrt(jnp.mean(packed * packed, axis=-1, keepdims=True) + 1e-05) * norm_gain
    ).astype(jnp.bfloat16)
    query = jnp.dot(normed, qkv_weight[0], preferred_element_type=jnp.float32).astype(jnp.bfloat16)
    keyed = jnp.dot(normed, qkv_weight[1], preferred_element_type=jnp.float32).astype(jnp.bfloat16)
    valued = jnp.dot(normed, qkv_weight[2], preferred_element_type=jnp.float32).astype(jnp.bfloat16)
    att_here = query.shape[1] // ATT_DIM
    queries = query.reshape(ROWS_DEV, att_here, ATT_DIM)
    row_place = first_row + jnp.arange(ROWS_DEV, dtype=jnp.int32)
    scale = ATT_DIM ** (-0.5)
    running = jnp.full((att_here, ROWS_DEV), -1e30, jnp.float32)
    key_piece = lax.all_gather(keyed, "seq", axis=0, tiled=True)
    value_piece = lax.all_gather(valued, "seq", axis=0, tiled=True)
    count = key_piece.shape[0]
    key_heads = key_piece.reshape(count, att_here, ATT_DIM)
    value_heads = value_piece.reshape(count, att_here, ATT_DIM)
    scores = (
        jnp.einsum("qhd,khd->hqk", queries, key_heads, preferred_element_type=jnp.float32) * scale
    )
    allowed = jnp.arange(count, dtype=jnp.int32)[None, :] <= row_place[:, None]
    scores = jnp.where(allowed[None], scores, -1e30)
    highest = jnp.maximum(running, jnp.max(scores, axis=-1))
    exps = jnp.where(allowed[None], jnp.exp(scores - highest[:, :, None]), 0.0)
    totals = jnp.sum(exps, axis=-1)
    weights = exps.astype(jnp.bfloat16)
    accum = jnp.einsum("hqk,khd->hqd", weights, value_heads, preferred_element_type=jnp.float32)
    running, totals, accum = (highest, totals, accum)
    result = accum / totals[:, :, None]
    return result.transpose(1, 0, 2).reshape(ROWS_DEV, att_here * ATT_DIM)


F32 = jnp.float32
BF16 = jnp.bfloat16
CHUNKS = 2


def exact_dot(a, b, dims=((1,), (0,))):
    return lax.dot_general(
        a, b, (dims, ((), ())), precision=lax.Precision.HIGHEST, preferred_element_type=F32
    )


def fast_dot(a, b, dims=((1,), (0,))):
    return lax.dot_general(a, b, (dims, ((), ())), preferred_element_type=F32)


def halves(a):
    high = a.astype(BF16)
    return high, (a - high.astype(F32)).astype(BF16)


def iota(shape, dim):
    return lax.broadcasted_iota(jnp.int32, shape, dim)


def fused(
    seqs,
    groups,
    decay_hbm,
    x_hbm,
    b_hbm,
    counts_hbm,
    bound_hbm,
    c_hbm,
    skip_hbm,
    outw_hbm,
    gain_hbm,
    qkvw_hbm,
    out_ref,
    decay_ref,
    x_ref,
    b_ref,
    counts_ref,
    bound_ref,
    c_ref,
    skip_ref,
    outw,
    gain_ref,
    qkvw,
    x_both,
    tag_send,
    tag_recv,
    send_a,
    recv_a,
    send_b,
    recv_b,
    send_w,
    recv_w,
    send_x,
    recv_x,
    send_p,
    recv_p,
    recv_n,
    send_q,
    recv_q,
    send_o,
    first_out,
    weight_sem,
    tag_sem,
    a_send,
    a_recv,
    b_send,
    b_recv,
    w_sem,
    x_send,
    x_recv,
    p_send,
    p_recv,
    n_sem,
    q_send,
    q_recv,
    o_send,
    o_recv,
    out_sem,
):
    me = lax.axis_index("seq")
    col = lax.axis_index("head")
    length, width = x_ref.shape
    heads = decay_ref.shape[0]
    lanes = width // heads
    pair_width = 2 * lanes
    pairs = heads // 2
    state = b_ref.shape[1]
    slots = bound_ref.shape[1]
    rows = out_ref.shape[0]
    half = rows // 2
    lo = (seqs - pairs) // 2
    is_owner = (me >= lo) & (me < lo + pairs)
    has_below, has_above = me > 0, me < seqs - 1

    def shard_at(d):
        return lax.rem(me + d + seqs, seqs)

    layers = seqs // 2
    mid = layers // 2
    layer, side = me // 2, lax.rem(me, 2)
    near_end = layer < mid
    far_layers = [jnp.where(near_end, layers - 1 - k, k) for k in range(layers - mid)]
    same = jnp.where(near_end, layer, layer - (layers - mid))
    for k in range(1, mid):
        turn = lax.rem(same + k, mid)
        far_layers.append(jnp.where(near_end, turn, turn + (layers - mid)))
    targets = []
    for there in far_layers + [layer]:
        targets.append(2 * there + 1 - side)
        if there is not layer:
            targets.append(2 * there + side)

    def head_at(d):
        return lax.rem(col + d, groups)

    chip = col // 2
    core = lax.rem(col, 2)
    partner = 2 * chip + 1 - core
    other = 2 * (1 - chip)

    barrier = pltpu.get_barrier_semaphore()
    peers = [(shard_at(d), col) for d in range(1, seqs)]
    peers += [(me, head_at(d)) for d in range(1, groups)]
    for peer in peers:
        pl.semaphore_signal(
            barrier, inc=1, device_id=peer, device_id_type=pl.DeviceIdType.MESH
        )

    def remote(src, dst, send_sem, recv_sem, peer):
        return pltpu.make_async_remote_copy(
            src_ref=src,
            dst_ref=dst,
            send_sem=send_sem,
            recv_sem=recv_sem,
            device_id=peer,
            device_id_type=pl.DeviceIdType.MESH,
        )

    loads = [
        pltpu.make_async_copy(source, target, weight_sem.at[i])
        for i, (source, target) in enumerate(
            (
                (decay_hbm, decay_ref),
                (x_hbm, x_ref),
                (b_hbm, b_ref),
                (counts_hbm, counts_ref),
                (bound_hbm, bound_ref),
                (c_hbm, c_ref),
                (skip_hbm, skip_ref),
                (outw_hbm, outw),
                (gain_hbm, gain_ref),
                (qkvw_hbm, qkvw),
            )
        )
    ]
    for load in loads[:7]:
        load.start()

    loads[0].wait()
    decay = decay_ref[...]
    upper = (iota((length, length), 0) <= iota((length, length), 1)).astype(F32)
    logs = -exact_dot(decay, upper)
    tail = jnp.exp(logs[:, length - 1 : length] - logs)
    loads[3].wait()
    tag_row = iota((heads, state), 1) == iota((heads, state), 0)
    tags = jnp.where(tag_row, logs[:, length - 1 : length], 0.0)
    tags = jnp.sum(tags, axis=0, keepdims=True)
    number = jnp.broadcast_to(counts_ref[...].astype(F32), (1, state))
    tag_send[...] = jnp.where(iota((1, state), 1) == heads, number, tags)
    loads[1].wait()
    loads[2].wait()
    for load in loads[7:]:
        load.start()
    b_turned = b_ref[...].T
    first_half = iota((state, pair_width), 1) < lanes
    for pair in range(pairs):
        x_high, x_low = halves(x_ref[:, pair * pair_width : (pair + 1) * pair_width])
        both = jnp.concatenate([x_high, x_low], axis=1)
        x_both[pair] = both
        faded = [b_turned * tail[h : h + 1, :] for h in (2 * pair, 2 * pair + 1)]
        f_high, f_low = halves(jnp.concatenate(faded, axis=0))
        wide = fast_dot(f_high, both)
        own = wide[:, :pair_width] + wide[:, pair_width:] + fast_dot(f_low, x_high)
        send_a[pair] = jnp.where(first_half, own[:state], own[state:]).astype(BF16)
    pl.semaphore_wait(barrier, len(peers))

    def tag_copy(to, slot, source):
        return remote(tag_send, tag_recv.at[slot], tag_sem.at[0, to], tag_sem.at[1, source], (to, col))

    def a_copy(j, slot):
        return remote(send_a.at[j], recv_a.at[slot], a_send.at[j], a_recv.at[slot], (lo + j, col))

    for to in targets:
        tag_copy(to, me, me).start()
    for k in range(pairs):
        j = jnp.where(near_end, pairs - 1 - k, k)

        @pl.when((me != lo + j) & (me < seqs - 1))
        def _():
            a_copy(j, me).start()

    tag_recv[me] = tag_send[...]

    @pl.when(is_owner)
    def _():
        recv_a[me] = send_a[me - lo]

    @pl.when(me == 0)
    def _():
        recv_b[...] = jnp.zeros(recv_b.shape, recv_b.dtype)

    lower = (iota((length, length), 0) >= iota((length, length), 1)).astype(F32)
    twice = [decay, decay, jnp.zeros((state - 2 * heads, length), F32)]
    logs_t = -exact_dot(lower, jnp.concatenate(twice, axis=0), ((1,), (1,)))
    lane = iota((state, width), 0)
    first = lax.rem(lane, heads) * lanes
    channel = iota((state, width), 1)
    spread = (channel >= first) & (channel < first + lanes)
    spread_one = (spread & (lane < heads)).astype(F32)
    spread_two = (spread & (lane < 2 * heads)).astype(BF16)
    for load in loads[4:7]:
        load.wait()
    marks = jnp.broadcast_to(bound_ref[...].astype(F32), (slots, slots)).T
    marks = jnp.concatenate([marks] * (length // slots), axis=1)
    place = iota((slots, length), 1).astype(F32)
    hit = place == marks
    seen = place <= marks
    onehot = hit.astype(F32)
    c_rows = exact_dot(onehot, c_ref[...])
    logs_sel = exact_dot(onehot, logs_t)
    affinity = exact_dot(c_rows, b_ref[...], ((1,), (1,)))
    inside = []
    first_lane = iota((slots, pair_width), 1) < lanes
    for pair in range(pairs):
        both = x_both[pair]
        parts = []
        for h in (2 * pair, 2 * pair + 1):
            gap = logs_sel[:, h : h + 1] - logs[h : h + 1, :]
            weights = jnp.where(seen, jnp.exp(jnp.where(seen, gap, 0.0)), 0.0) * affinity
            weights = weights + jnp.where(hit, skip_ref[:, h : h + 1], 0.0)
            w_high, w_low = halves(weights)
            wide = fast_dot(w_high, both)
            parts.append(
                wide[:, :pair_width] + wide[:, pair_width:] + fast_dot(w_low, both[:, :pair_width])
            )
        inside.append(jnp.where(first_lane, parts[0], parts[1]))
    inside = jnp.concatenate(inside, axis=1)
    enter = jnp.exp(logs_sel)
    e_high = enter.astype(BF16).astype(F32)
    enter_lane = iota((slots, state), 1)
    e_pack = jnp.where(enter_lane < heads, e_high, enter - e_high)
    e_pack = jnp.where(enter_lane < 2 * heads, e_pack, 0.0).astype(BF16)
    sel = jnp.concatenate([*halves(inside), *halves(c_rows), e_pack], axis=1)

    for d in range(1, seqs):
        source = shard_at(-d)
        tag_copy(shard_at(d), source, source).wait_recv()
    all_tags = tag_recv[...].reshape(seqs, state)
    tag_lane = iota((seqs, state), 1)
    tag_shard = iota((seqs, state), 0)
    earlier = (tag_shard < me) & (tag_lane == heads)
    start = jnp.sum(jnp.where(earlier, all_tags, 0.0), axis=(0, 1), keepdims=True)
    offset = start - (me * rows - half).astype(F32)
    slot = iota((slots, slots), 1).astype(F32)
    count = jnp.broadcast_to(counts_ref[...].astype(F32), (slots, slots))
    shift = (slot == iota((slots, slots), 0).astype(F32) - offset) & (slot < count)
    window = fast_dot(shift.astype(BF16), sel)
    send_w[...] = jnp.concatenate(
        [window[:rows, :width], window[:rows, 2 * width :]], axis=1
    ).astype(BF16)

    w_copy = remote(send_w, recv_w, w_sem.at[0], w_sem.at[1], (shard_at(-1), col))

    @pl.when(has_below)
    def _():
        w_copy.start()

    @pl.when(jnp.logical_not(has_above))
    def _():
        recv_w[...] = jnp.zeros(recv_w.shape, recv_w.dtype)

    for load in loads[7:]:
        load.wait()

    def norm(parts):
        mixed = parts[0].astype(F32)
        for k in range(1, groups):
            mixed = mixed + parts[k].astype(F32)
        square = jnp.mean(mixed * mixed, axis=-1, keepdims=True)
        return (mixed * lax.rsqrt(square + 1e-05) * gain_ref[...]).astype(BF16)

    def q_copy(j, block, part):
        return remote(
            send_q.at[j, part], recv_q.at[block], q_send.at[part, j], q_recv.at[block], (lo + j, col)
        )

    def spread_out(block, to, part):
        for i in range(3):
            product = fast_dot(block, qkvw[i]).astype(BF16)
            for pair in range(pairs):
                send_q[pair, part, i] = product[:, pair * pair_width : (pair + 1) * pair_width]
        for k in range(pairs):
            j = jnp.where(near_end, pairs - 1 - k, k)

            @pl.when((me != lo + j) & (to < 2 * seqs))
            def _():
                q_copy(j, to, part).start()

    def x_copy(k, slot, to):
        return remote(send_x, recv_x.at[slot], x_send.at[k], x_recv.at[slot], (me, to))

    @pl.when(me == 0)
    def _():
        early = window[half:rows, :width] + window[half:rows, width : 2 * width]
        send_x[...] = fast_dot(early.astype(BF16), outw[...]).astype(BF16)
        for k, to in enumerate((other, other + 1, partner)):
            x_copy(k, col, to).start()
        recv_x[col] = send_x[...]
        for k, source in enumerate((partner, other, other + 1)):
            x_copy(0, source, source).wait_recv()
        spread_out(norm(recv_x), 0, 2)

    def b_copy(s, j):
        return remote(send_b.at[s], recv_b.at[j], b_send.at[s], b_recv.at[j], (s, col))

    @pl.when(is_owner)
    def _():
        mine = me - lo
        even = jnp.sum(jnp.where(tag_lane == 2 * mine, all_tags, 0.0), axis=1, keepdims=True)
        odd = jnp.sum(jnp.where(tag_lane == 2 * mine + 1, all_tags, 0.0), axis=1, keepdims=True)
        kept = jnp.exp(jnp.where(iota((seqs, pair_width), 1) < lanes, even, odd))
        running = jnp.zeros((state, pair_width), F32)
        for s in range(1, seqs):

            @pl.when(me != s - 1)
            def _():
                a_copy(mine, s - 1).wait_recv()

            running = kept[s - 1 : s] * running + recv_a[s - 1].astype(F32)
            send_b[s] = running.astype(BF16)

            @pl.when(me != s)
            def _():
                b_copy(s, mine).start()

        recv_b[mine] = send_b[me]

    spans = jnp.exp(jnp.where(tag_lane < heads, all_tags, 0.0))
    here = jnp.sum(jnp.where(tag_shard == me, spans, 0.0), axis=0, keepdims=True)
    span_here = exact_dot(jnp.broadcast_to(here, (heads, state)), spread_one)[0:1]
    owned = window[rows:]
    mine_scale = fast_dot(owned[:, 2 * width + 2 * state :].astype(BF16), spread_two)

    @pl.when(has_above)
    def _():
        w_copy.wait_recv()

    near_rows = recv_w[...].astype(F32)
    near_scale = fast_dot(recv_w[:, width + 2 * state :], spread_two)
    c_both = owned[:, 2 * width : 2 * width + 2 * state] + near_rows[:, width : width + 2 * state]
    c_stack = jnp.concatenate([c_both[:, :state], c_both[:, state:]], axis=0).astype(BF16)

    def through(ref):
        wide = fast_dot(c_stack, jnp.concatenate([ref[j] for j in range(pairs)], axis=1))
        return wide[:rows] + wide[rows:]

    reach = owned[:, :width] + owned[:, width : 2 * width] + near_rows[:, :width]
    reach = reach + near_scale * through(send_a)
    far_scale = mine_scale + span_here * near_scale

    for j in range(pairs):

        @pl.when(has_below & (me != lo + j))
        def _():
            b_copy(me, j).wait_recv()

    y = (reach + far_scale * through(recv_b)).astype(BF16)
    partial = fast_dot(y, outw[...]).astype(BF16)
    for part in range(CHUNKS):
        send_p[part] = partial[part * half : (part + 1) * half]

    def p_copy(src, slot, k, to):
        return remote(send_p.at[src], recv_p.at[slot], p_send.at[k], p_recv.at[slot], (me, to))

    sent = [
        p_copy(0, col, 0, other),
        p_copy(1, col, 1, other + 1),
        p_copy(1 - core, col, 2, partner),
    ]
    for copy in sent:
        copy.start()
    recv_p[col] = send_p[core]
    for source in (partner, other, other + 1):
        p_copy(0, source, 0, source).wait_recv()
    normed = norm(recv_p)
    recv_n[core] = normed

    def n_copy(slot):
        return remote(recv_n.at[core], recv_n.at[slot], n_sem.at[0], n_sem.at[1], (me, partner))

    n_copy(core).start()
    spread_out(normed, 2 * me + 1 + core, core)
    n_copy(1 - core).wait_recv()
    spread_out(recv_n[1 - core], 2 * me + 2 - core, 1 - core)

    def attend(queries, keys, values):
        count, seen_before = queries.shape[0], keys.shape[0] - queries.shape[0]
        left = iota(queries.shape, 1) < lanes
        scaled = queries.astype(F32) * (lanes ** (-0.5))
        heads_apart = [jnp.where(left, scaled, 0.0), jnp.where(left, 0.0, scaled)]
        stacked = jnp.concatenate(heads_apart, axis=0).astype(BF16)
        scores = fast_dot(stacked, keys, ((1,), (1,)))
        corner = (2 * count, count)
        row = iota(corner, 0)
        row = jnp.where(row < count, row, row - count)
        last = jnp.where(row >= iota(corner, 1), scores[:, seen_before:], -1e30)
        highest = jnp.max(last, axis=-1, keepdims=True)
        if seen_before:
            first = scores[:, :seen_before]
            highest = jnp.maximum(highest, jnp.max(first, axis=-1, keepdims=True))
        exps = jnp.exp(last - highest)
        total = jnp.sum(exps, axis=-1, keepdims=True)
        result = fast_dot(exps.astype(BF16), values[seen_before:])
        if seen_before:
            exps = jnp.exp(first - highest)
            total = total + jnp.sum(exps, axis=-1, keepdims=True)
            result = result + fast_dot(exps.astype(BF16), values[:seen_before])
        result = result / total
        return jnp.where(left, result[:count], result[count:]).astype(BF16)

    @pl.when(me == 0)
    def _():
        for pair in range(pairs):
            q, k, v = [
                jnp.concatenate([send_q[pair, 2, i], send_q[pair, 0, i]], axis=0) for i in range(3)
            ]
            first_out[:, pair * pair_width : (pair + 1) * pair_width] = attend(q, k, v)
        pltpu.make_async_copy(first_out, out_ref, out_sem).start()

    def o_copy(s, j):
        place = pl.ds(pl.multiple_of(j * pair_width, pair_width), pair_width)
        return remote(send_o.at[s], out_ref.at[:, place], o_send.at[s], o_recv.at[j], (s, col))

    def o_keep(j):
        place = pl.ds(pl.multiple_of(j * pair_width, pair_width), pair_width)
        return pltpu.make_async_copy(send_o.at[me], out_ref.at[:, place], out_sem)

    @pl.when(is_owner)
    def _():
        mine = me - lo
        for part in range(CHUNKS):
            recv_q[2 * me + 1 + part] = send_q[mine, part]
        for block in range(2 * seqs):

            @pl.when(me != max(block - 1, 0) // 2)
            def _():
                q_copy(mine, block, 0).wait_recv()

        q, k, v = [recv_q[:, i].reshape(seqs * rows, pair_width) for i in range(3)]
        span = 2 * rows
        for n in [0, seqs // 2 - 1, *range(1, seqs // 2 - 1)]:
            end = (n + 1) * span
            result = attend(q[n * span : end], k[:end], v[:end])
            for s in (2 * n, 2 * n + 1):
                if s == 0:
                    continue
                send_o[s] = result[(s - 2 * n) * rows : (s - 2 * n + 1) * rows]

                @pl.when(me != s)
                def _():
                    o_copy(s, mine).start()

        o_keep(mine).start()
        o_keep(mine).wait()

    @pl.when(me == 0)
    def _():
        pltpu.make_async_copy(first_out, out_ref, out_sem).wait()

    for j in range(pairs):

        @pl.when((me > 0) & (me != lo + j))
        def _():
            o_copy(me, j).wait_recv()

    for copy in sent:
        copy.wait_send()
    n_copy(core).wait_send()

    @pl.when(has_below)
    def _():
        w_copy.wait_send()

    @pl.when(me == 0)
    def _():
        for k in range(3):
            x_copy(k, col, partner).wait_send()
        for j in range(pairs):
            q_copy(j, 0, 2).wait_send()

    for j in range(pairs):

        @pl.when((me != lo + j) & (me < seqs - 1))
        def _():
            a_copy(j, me).wait_send()

        @pl.when(me != lo + j)
        def _():
            q_copy(j, 0, 0).wait_send()

        @pl.when((me != lo + j) & has_above)
        def _():
            q_copy(j, 0, 1).wait_send()

    for to in targets:
        tag_copy(to, me, me).wait_send()

    for s in range(1, seqs):

        @pl.when(is_owner & (me != s))
        def _():
            b_copy(s, me - lo).wait_send()
            o_copy(s, me - lo).wait_send()


def fused_body(
    byte_input,
    b_proj,
    c_proj,
    step_decay,
    skip_gain,
    out_weight,
    boundaries,
    counts,
    norm_gain,
    qkv_weight,
):
    seqs, groups = lax.axis_size("seq"), lax.axis_size("head")
    heads = step_decay.shape[0]
    length, width = byte_input.shape
    lanes = width // heads
    pairs = heads // 2
    state = b_proj.shape[1]
    rows = ROWS_DEV
    half = rows // 2
    enc = out_weight.shape[1]
    hbm = pl.BlockSpec(memory_space=pl.ANY)
    dma = pltpu.SemaphoreType.DMA
    operands = (
        step_decay,
        byte_input,
        b_proj,
        counts.reshape(1, 1),
        boundaries,
        c_proj,
        skip_gain.reshape(1, -1),
        out_weight,
        norm_gain.reshape(1, -1),
        qkv_weight,
    )
    result = pl.pallas_call(
        functools.partial(fused, seqs, groups),
        out_shape=jax.ShapeDtypeStruct((rows, width), BF16),
        in_specs=[hbm] * len(operands),
        out_specs=hbm,
        scratch_shapes=[pltpu.VMEM(array.shape, array.dtype) for array in operands]
        + [
            pltpu.VMEM((pairs, length, 4 * lanes), BF16),
            pltpu.VMEM((1, state), F32),
            pltpu.VMEM((seqs, 1, state), F32),
            pltpu.VMEM((pairs, state, 2 * lanes), BF16),
            pltpu.VMEM((seqs, state, 2 * lanes), BF16),
            pltpu.VMEM((seqs, state, 2 * lanes), BF16),
            pltpu.VMEM((pairs, state, 2 * lanes), BF16),
            pltpu.VMEM((rows, width + 3 * state), BF16),
            pltpu.VMEM((rows, width + 3 * state), BF16),
            pltpu.VMEM((half, enc), BF16),
            pltpu.VMEM((groups, half, enc), BF16),
            pltpu.VMEM((CHUNKS, half, enc), BF16),
            pltpu.VMEM((groups, half, enc), BF16),
            pltpu.VMEM((CHUNKS, half, enc), BF16),
            pltpu.VMEM((pairs, CHUNKS + 1, 3, half, 2 * lanes), BF16),
            pltpu.VMEM((seqs * CHUNKS, 3, half, 2 * lanes), BF16),
            pltpu.VMEM((seqs, rows, 2 * lanes), BF16),
            pltpu.VMEM((rows, width), BF16),
            dma((len(operands),)),
            dma((2, seqs)),
            dma((pairs,)),
            dma((seqs,)),
            dma((seqs,)),
            dma((pairs,)),
            dma((2,)),
            dma((groups,)),
            dma((groups,)),
            dma((groups,)),
            dma((groups,)),
            dma((2,)),
            dma((CHUNKS + 1, pairs)),
            dma((CHUNKS * seqs,)),
            dma((seqs,)),
            dma((pairs,)),
            dma,
        ],
        compiler_params=pltpu.CompilerParams(collective_id=0, has_side_effects=True),
    )(*operands)
    return result.astype(F32)


def chosen(*args):
    byte_input, step_decay, slots = args[0], args[3], args[6].shape[1]
    heads = step_decay.shape[0]
    lanes = byte_input.shape[1] // heads
    seqs, groups = lax.axis_size("seq"), lax.axis_size("head")
    fits = seqs == heads and lanes == ATT_DIM and args[9].shape[2] == byte_input.shape[1]
    fits = fits and 2 * lanes == slots and args[1].shape[1] == slots and slots == 2 * ROWS_DEV
    fits = fits and seqs % 4 == 0 and groups == 2 * CHUNKS and ROWS_DEV % (16 * groups) == 0
    fits = fits and byte_input.shape[0] % slots == 0
    return fused_body(*args) if fits else body(*args)


def solution(mesh):
    return jax.shard_map(
        chosen,
        mesh=mesh,
        in_specs=(
            P("seq", "head"),
            P("seq", None),
            P("seq", None),
            P("head", "seq"),
            P("head"),
            P("head", None),
            P("seq", None),
            P("seq"),
            P(),
            P(None, None, "head"),
        ),
        out_specs=P("seq", "head"),
        check_vma=False,
    )
```

```python
import functools

import jax
import jax.numpy as jnp
from jax import lax
from jax.experimental import pallas as pl
from jax.experimental.pallas import tpu as pltpu
from jax.sharding import PartitionSpec as P

ATT_DIM = 64
ROWS_DEV = 64


def prefix(shard, axis, combine, identity):
    length, here = (lax.axis_size(axis), lax.axis_index(axis))
    everything = jax.tree.map(lambda part: lax.all_gather(part, axis), shard)
    start = jax.tree.map(
        lambda part, zero: jnp.broadcast_to(jnp.asarray(zero, part.dtype), part.shape),
        shard,
        identity,
    )

    def lap(k, before):
        reached = k < here
        new = combine(before, jax.tree.map(lambda part: part[k], everything))
        return jax.tree.map(lambda a, b: jnp.where(reached, a, b), new, before)

    return lax.fori_loop(0, length, lap, start)


def extended(cells, sides, width):
    for axis, dim in sides:
        count = lax.axis_size(axis)
        ends = count - 1
        head = lax.slice_in_dim(cells, 0, width, axis=dim)
        tail = lax.slice_in_dim(cells, cells.shape[dim] - width, cells.shape[dim], axis=dim)
        cells = jnp.concatenate(
            [
                lax.ppermute(tail, axis, [(i, (i + 1) % count) for i in range(ends)]),
                cells,
                lax.ppermute(head, axis, [((i + 1) % count, i) for i in range(ends)]),
            ],
            axis=dim,
        )
    return cells


def state_space(inputs, b_rows, c_rows, decay):
    log_decay = jnp.cumsum(-decay, axis=1)
    affinity = jnp.dot(c_rows, b_rows.T, precision=lax.Precision.HIGHEST)
    length = inputs.shape[0]
    causal = lax.broadcasted_iota(jnp.int32, (length, length), 0) >= lax.broadcasted_iota(
        jnp.int32, (length, length), 1
    )

    def one_head(pair):
        values, logs = pair
        weights = (
            jnp.where(causal, jnp.exp(jnp.where(causal, logs[:, None] - logs[None, :], 0.0)), 0.0)
            * affinity
        )
        return jnp.dot(weights, values, precision=lax.Precision.HIGHEST)

    inside = lax.map(one_head, (inputs.transpose(1, 0, 2), log_decay))
    tail = jnp.exp(log_decay[:, -1:] - log_decay)
    own_state = jnp.einsum("ht,thp,tn->hpn", tail, inputs, b_rows, precision=lax.Precision.HIGHEST)
    return (log_decay, inside, own_state)


def link(earlier, later):
    return (earlier[0] * later[0], later[0][:, None, None] * earlier[1] + later[1])


def body(
    byte_input,
    b_proj,
    c_proj,
    step_decay,
    skip_gain,
    out_weight,
    boundaries,
    counts,
    norm_gain,
    qkv_weight,
):
    heads_here = step_decay.shape[0]
    length = byte_input.shape[0]
    inputs = byte_input.reshape(length, heads_here, -1)
    log_decay, inside, own_state = state_space(inputs, b_proj, c_proj, step_decay)
    span_decay = jnp.exp(log_decay[:, -1])
    arriving = prefix(
        (span_decay, own_state), "seq", link, (jnp.ones_like(span_decay), jnp.zeros_like(own_state))
    )
    carried = jnp.exp(log_decay)[:, :, None] * jnp.einsum(
        "tn,hpn->htp", c_proj, arriving[1], precision=lax.Precision.HIGHEST
    )
    mixed_heads = inside + carried + skip_gain[:, None, None] * inputs.transpose(1, 0, 2)
    slots = boundaries.shape[1]
    picked = jnp.take(mixed_heads, boundaries[0], axis=1)
    selected = picked.transpose(1, 0, 2).reshape(slots, -1).astype(jnp.bfloat16)
    all_counts = lax.all_gather(counts, "seq", axis=0, tiled=True)
    starts = jnp.cumsum(all_counts) - all_counts
    myself = lax.axis_index("seq")
    shards = lax.axis_size("seq")
    slot = jnp.arange(slots, dtype=jnp.int32)

    def slot_index(source):
        inside_axis = (source >= 0) & (source < shards)
        safe = jnp.clip(source, 0, shards - 1)
        begin = jnp.take(starts, safe)
        number = jnp.take(all_counts, safe)
        return jnp.where(inside_axis & (slot < number), begin + slot, -1)

    global_index = jnp.concatenate(
        [slot_index(myself - 1), slot_index(myself), slot_index(myself + 1)]
    )
    first_row = myself * ROWS_DEV
    target = first_row + jnp.arange(ROWS_DEV, dtype=jnp.int32)
    picker = global_index[None, :] == target[:, None]
    nearby = extended(selected, (("seq", 0),), slots)
    owned = jnp.dot(picker.astype(jnp.bfloat16), nearby, preferred_element_type=jnp.float32).astype(
        jnp.bfloat16
    )
    partial_value = jnp.dot(owned, out_weight, preferred_element_type=jnp.float32)
    packed = lax.psum(partial_value, "head")
    normed = (
        packed * lax.rsqrt(jnp.mean(packed * packed, axis=-1, keepdims=True) + 1e-05) * norm_gain
    ).astype(jnp.bfloat16)
    query = jnp.dot(normed, qkv_weight[0], preferred_element_type=jnp.float32).astype(jnp.bfloat16)
    keyed = jnp.dot(normed, qkv_weight[1], preferred_element_type=jnp.float32).astype(jnp.bfloat16)
    valued = jnp.dot(normed, qkv_weight[2], preferred_element_type=jnp.float32).astype(jnp.bfloat16)
    att_here = query.shape[1] // ATT_DIM
    queries = query.reshape(ROWS_DEV, att_here, ATT_DIM)
    row_place = first_row + jnp.arange(ROWS_DEV, dtype=jnp.int32)
    scale = ATT_DIM ** (-0.5)
    running = jnp.full((att_here, ROWS_DEV), -1e30, jnp.float32)
    key_piece = lax.all_gather(keyed, "seq", axis=0, tiled=True)
    value_piece = lax.all_gather(valued, "seq", axis=0, tiled=True)
    count = key_piece.shape[0]
    key_heads = key_piece.reshape(count, att_here, ATT_DIM)
    value_heads = value_piece.reshape(count, att_here, ATT_DIM)
    scores = (
        jnp.einsum("qhd,khd->hqk", queries, key_heads, preferred_element_type=jnp.float32) * scale
    )
    allowed = jnp.arange(count, dtype=jnp.int32)[None, :] <= row_place[:, None]
    scores = jnp.where(allowed[None], scores, -1e30)
    highest = jnp.maximum(running, jnp.max(scores, axis=-1))
    exps = jnp.where(allowed[None], jnp.exp(scores - highest[:, :, None]), 0.0)
    totals = jnp.sum(exps, axis=-1)
    weights = exps.astype(jnp.bfloat16)
    accum = jnp.einsum("hqk,khd->hqd", weights, value_heads, preferred_element_type=jnp.float32)
    running, totals, accum = (highest, totals, accum)
    result = accum / totals[:, :, None]
    return result.transpose(1, 0, 2).reshape(ROWS_DEV, att_here * ATT_DIM)


F32 = jnp.float32
BF16 = jnp.bfloat16
CHUNKS = 2


def exact_dot(a, b, dims=((1,), (0,))):
    return lax.dot_general(
        a, b, (dims, ((), ())), precision=lax.Precision.HIGHEST, preferred_element_type=F32
    )


def fast_dot(a, b, dims=((1,), (0,))):
    return lax.dot_general(a, b, (dims, ((), ())), preferred_element_type=F32)


def halves(a):
    high = a.astype(BF16)
    return high, (a - high.astype(F32)).astype(BF16)


def iota(shape, dim):
    return lax.broadcasted_iota(jnp.int32, shape, dim)


def fused(
    seqs,
    groups,
    decay_hbm,
    x_hbm,
    b_hbm,
    counts_hbm,
    bound_hbm,
    c_hbm,
    skip_hbm,
    outw_hbm,
    gain_hbm,
    qkvw_hbm,
    out_ref,
    decay_ref,
    x_ref,
    b_ref,
    counts_ref,
    bound_ref,
    c_ref,
    skip_ref,
    outw,
    gain_ref,
    qkvw,
    x_both,
    tag_send,
    tag_recv,
    send_a,
    recv_a,
    send_b,
    recv_b,
    send_w,
    recv_w,
    send_x,
    recv_x,
    send_p,
    recv_p,
    recv_n,
    send_q,
    recv_q,
    send_o,
    first_out,
    weight_sem,
    tag_sem,
    a_send,
    a_recv,
    b_send,
    b_recv,
    w_sem,
    x_send,
    x_recv,
    p_send,
    p_recv,
    n_sem,
    q_send,
    q_recv,
    o_send,
    o_recv,
    out_sem,
):
    me = lax.axis_index("seq")
    col = lax.axis_index("head")
    length, width = x_ref.shape
    heads = decay_ref.shape[0]
    lanes = width // heads
    pair_width = 2 * lanes
    pairs = heads // 2
    state = b_ref.shape[1]
    slots = bound_ref.shape[1]
    rows = out_ref.shape[0]
    half = rows // 2
    lo = (seqs - pairs) // 2
    is_owner = (me >= lo) & (me < lo + pairs)
    has_below, has_above = me > 0, me < seqs - 1

    def shard_at(d):
        return lax.rem(me + d + seqs, seqs)

    layers = seqs // 2
    mid = layers // 2
    layer, side = me // 2, lax.rem(me, 2)
    near_end = layer < mid
    far_layers = [jnp.where(near_end, layers - 1 - k, k) for k in range(layers - mid)]
    same = jnp.where(near_end, layer, layer - (layers - mid))
    for k in range(1, mid):
        turn = lax.rem(same + k, mid)
        far_layers.append(jnp.where(near_end, turn, turn + (layers - mid)))
    targets = []
    for there in far_layers + [layer]:
        targets.append(2 * there + 1 - side)
        if there is not layer:
            targets.append(2 * there + side)

    def head_at(d):
        return lax.rem(col + d, groups)

    chip = col // 2
    core = lax.rem(col, 2)
    partner = 2 * chip + 1 - core
    other = 2 * (1 - chip)

    barrier = pltpu.get_barrier_semaphore()
    peers = [(shard_at(d), col) for d in range(1, seqs)]
    peers += [(me, head_at(d)) for d in range(1, groups)]
    for peer in peers:
        pl.semaphore_signal(
            barrier, inc=1, device_id=peer, device_id_type=pl.DeviceIdType.MESH
        )

    def remote(src, dst, send_sem, recv_sem, peer):
        return pltpu.make_async_remote_copy(
            src_ref=src,
            dst_ref=dst,
            send_sem=send_sem,
            recv_sem=recv_sem,
            device_id=peer,
            device_id_type=pl.DeviceIdType.MESH,
        )

    loads = [
        pltpu.make_async_copy(source, target, weight_sem.at[i])
        for i, (source, target) in enumerate(
            (
                (decay_hbm, decay_ref),
                (x_hbm, x_ref),
                (b_hbm, b_ref),
                (counts_hbm, counts_ref),
                (bound_hbm, bound_ref),
                (c_hbm, c_ref),
                (skip_hbm, skip_ref),
                (outw_hbm, outw),
                (gain_hbm, gain_ref),
                (qkvw_hbm, qkvw),
            )
        )
    ]
    for load in loads[:7]:
        load.start()

    loads[0].wait()
    decay = decay_ref[...]
    upper = (iota((length, length), 0) <= iota((length, length), 1)).astype(F32)
    logs = -exact_dot(decay, upper)
    tail = jnp.exp(logs[:, length - 1 : length] - logs)
    loads[3].wait()
    tag_row = iota((heads, state), 1) == iota((heads, state), 0)
    tags = jnp.where(tag_row, logs[:, length - 1 : length], 0.0)
    tags = jnp.sum(tags, axis=0, keepdims=True)
    number = jnp.broadcast_to(counts_ref[...].astype(F32), (1, state))
    tag_send[...] = jnp.where(iota((1, state), 1) == heads, number, tags)
    loads[1].wait()
    loads[2].wait()
    for load in loads[7:]:
        load.start()
    b_turned = b_ref[...].T
    first_half = iota((state, pair_width), 1) < lanes
    for pair in range(pairs):
        x_high, x_low = halves(x_ref[:, pair * pair_width : (pair + 1) * pair_width])
        both = jnp.concatenate([x_high, x_low], axis=1)
        x_both[pair] = both
        faded = [b_turned * tail[h : h + 1, :] for h in (2 * pair, 2 * pair + 1)]
        f_high, f_low = halves(jnp.concatenate(faded, axis=0))
        wide = fast_dot(f_high, both)
        own = wide[:, :pair_width] + wide[:, pair_width:] + fast_dot(f_low, x_high)
        send_a[pair] = jnp.where(first_half, own[:state], own[state:]).astype(BF16)
    pl.semaphore_wait(barrier, len(peers))

    def tag_copy(to, slot, source):
        return remote(tag_send, tag_recv.at[slot], tag_sem.at[0, to], tag_sem.at[1, source], (to, col))

    def a_copy(j, slot):
        return remote(send_a.at[j], recv_a.at[slot], a_send.at[j], a_recv.at[slot], (lo + j, col))

    for to in targets:
        tag_copy(to, me, me).start()
    for k in range(pairs):
        j = jnp.where(near_end, pairs - 1 - k, k)

        @pl.when((me != lo + j) & (me < seqs - 1))
        def _():
            a_copy(j, me).start()

    tag_recv[me] = tag_send[...]

    @pl.when(is_owner)
    def _():
        recv_a[me] = send_a[me - lo]

    @pl.when(me == 0)
    def _():
        recv_b[...] = jnp.zeros(recv_b.shape, recv_b.dtype)

    lower = (iota((length, length), 0) >= iota((length, length), 1)).astype(F32)
    twice = [decay, decay, jnp.zeros((state - 2 * heads, length), F32)]
    logs_t = -exact_dot(lower, jnp.concatenate(twice, axis=0), ((1,), (1,)))
    lane = iota((state, width), 0)
    first = lax.rem(lane, heads) * lanes
    channel = iota((state, width), 1)
    spread = (channel >= first) & (channel < first + lanes)
    spread_one = (spread & (lane < heads)).astype(F32)
    spread_two = (spread & (lane < 2 * heads)).astype(BF16)
    for load in loads[4:7]:
        load.wait()
    marks = jnp.broadcast_to(bound_ref[...].astype(F32), (slots, slots)).T
    marks = jnp.concatenate([marks] * (length // slots), axis=1)
    place = iota((slots, length), 1).astype(F32)
    hit = place == marks
    seen = place <= marks
    onehot = hit.astype(F32)
    c_rows = exact_dot(onehot, c_ref[...])
    logs_sel = exact_dot(onehot, logs_t)
    affinity = exact_dot(c_rows, b_ref[...], ((1,), (1,)))
    inside = []
    first_lane = iota((slots, pair_width), 1) < lanes
    for pair in range(pairs):
        both = x_both[pair]
        parts = []
        for h in (2 * pair, 2 * pair + 1):
            gap = logs_sel[:, h : h + 1] - logs[h : h + 1, :]
            weights = jnp.where(seen, jnp.exp(jnp.where(seen, gap, 0.0)), 0.0) * affinity
            weights = weights + jnp.where(hit, skip_ref[:, h : h + 1], 0.0)
            w_high, w_low = halves(weights)
            wide = fast_dot(w_high, both)
            parts.append(
                wide[:, :pair_width] + wide[:, pair_width:] + fast_dot(w_low, both[:, :pair_width])
            )
        inside.append(jnp.where(first_lane, parts[0], parts[1]))
    inside = jnp.concatenate(inside, axis=1)
    enter = jnp.exp(logs_sel)
    e_high = enter.astype(BF16).astype(F32)
    enter_lane = iota((slots, state), 1)
    e_pack = jnp.where(enter_lane < heads, e_high, enter - e_high)
    e_pack = jnp.where(enter_lane < 2 * heads, e_pack, 0.0).astype(BF16)
    sel = jnp.concatenate([*halves(inside), *halves(c_rows), e_pack], axis=1)

    for d in range(1, seqs):
        source = shard_at(-d)
        tag_copy(shard_at(d), source, source).wait_recv()
    all_tags = tag_recv[...].reshape(seqs, state)
    tag_lane = iota((seqs, state), 1)
    tag_shard = iota((seqs, state), 0)
    earlier = (tag_shard < me) & (tag_lane == heads)
    start = jnp.sum(jnp.where(earlier, all_tags, 0.0), axis=(0, 1), keepdims=True)
    offset = start - (me * rows - half).astype(F32)
    slot = iota((slots, slots), 1).astype(F32)
    count = jnp.broadcast_to(counts_ref[...].astype(F32), (slots, slots))
    shift = (slot == iota((slots, slots), 0).astype(F32) - offset) & (slot < count)
    window = fast_dot(shift.astype(BF16), sel)
    send_w[...] = jnp.concatenate(
        [window[:rows, :width], window[:rows, 2 * width :]], axis=1
    ).astype(BF16)

    w_copy = remote(send_w, recv_w, w_sem.at[0], w_sem.at[1], (shard_at(-1), col))

    @pl.when(has_below)
    def _():
        w_copy.start()

    @pl.when(jnp.logical_not(has_above))
    def _():
        recv_w[...] = jnp.zeros(recv_w.shape, recv_w.dtype)

    for load in loads[7:]:
        load.wait()

    def norm(parts):
        mixed = parts[0].astype(F32)
        for k in range(1, groups):
            mixed = mixed + parts[k].astype(F32)
        square = jnp.mean(mixed * mixed, axis=-1, keepdims=True)
        return (mixed * lax.rsqrt(square + 1e-05) * gain_ref[...]).astype(BF16)

    def q_copy(j, block, part):
        return remote(
            send_q.at[j, part], recv_q.at[block], q_send.at[part, j], q_recv.at[block], (lo + j, col)
        )

    def spread_out(block, to, part):
        for i in range(3):
            product = fast_dot(block, qkvw[i]).astype(BF16)
            for pair in range(pairs):
                send_q[pair, part, i] = product[:, pair * pair_width : (pair + 1) * pair_width]
        for k in range(pairs):
            j = jnp.where(near_end, pairs - 1 - k, k)

            @pl.when((me != lo + j) & (to < 2 * seqs))
            def _():
                q_copy(j, to, part).start()

    def x_copy(k, slot, to):
        return remote(send_x, recv_x.at[slot], x_send.at[k], x_recv.at[slot], (me, to))

    @pl.when(me == 0)
    def _():
        early = window[half:rows, :width] + window[half:rows, width : 2 * width]
        send_x[...] = fast_dot(early.astype(BF16), outw[...]).astype(BF16)
        for k, to in enumerate((other, other + 1, partner)):
            x_copy(k, col, to).start()
        recv_x[col] = send_x[...]

    def b_copy(s, j):
        return remote(send_b.at[s], recv_b.at[j], b_send.at[s], b_recv.at[j], (s, col))

    @pl.when(is_owner)
    def _():
        mine = me - lo
        even = jnp.sum(jnp.where(tag_lane == 2 * mine, all_tags, 0.0), axis=1, keepdims=True)
        odd = jnp.sum(jnp.where(tag_lane == 2 * mine + 1, all_tags, 0.0), axis=1, keepdims=True)
        kept = jnp.exp(jnp.where(iota((seqs, pair_width), 1) < lanes, even, odd))
        running = jnp.zeros((state, pair_width), F32)
        for s in range(1, seqs):

            @pl.when(me != s - 1)
            def _():
                a_copy(mine, s - 1).wait_recv()

            running = kept[s - 1 : s] * running + recv_a[s - 1].astype(F32)
            send_b[s] = running.astype(BF16)

            @pl.when(me != s)
            def _():
                b_copy(s, mine).start()

        recv_b[mine] = send_b[me]

    spans = jnp.exp(jnp.where(tag_lane < heads, all_tags, 0.0))
    here = jnp.sum(jnp.where(tag_shard == me, spans, 0.0), axis=0, keepdims=True)
    span_here = exact_dot(jnp.broadcast_to(here, (heads, state)), spread_one)[0:1]
    owned = window[rows:]
    mine_scale = fast_dot(owned[:, 2 * width + 2 * state :].astype(BF16), spread_two)

    @pl.when(has_above)
    def _():
        w_copy.wait_recv()

    near_rows = recv_w[...].astype(F32)
    near_scale = fast_dot(recv_w[:, width + 2 * state :], spread_two)
    c_both = owned[:, 2 * width : 2 * width + 2 * state] + near_rows[:, width : width + 2 * state]
    c_stack = jnp.concatenate([c_both[:, :state], c_both[:, state:]], axis=0).astype(BF16)

    def through(ref):
        wide = fast_dot(c_stack, jnp.concatenate([ref[j] for j in range(pairs)], axis=1))
        return wide[:rows] + wide[rows:]

    reach = owned[:, :width] + owned[:, width : 2 * width] + near_rows[:, :width]
    reach = reach + near_scale * through(send_a)
    far_scale = mine_scale + span_here * near_scale

    for j in range(pairs):

        @pl.when(has_below & (me != lo + j))
        def _():
            b_copy(me, j).wait_recv()

    y = (reach + far_scale * through(recv_b)).astype(BF16)
    partial = fast_dot(y, outw[...]).astype(BF16)
    for part in range(CHUNKS):
        send_p[part] = partial[part * half : (part + 1) * half]

    def p_copy(part, slot, k, to):
        return remote(
            send_p.at[part], recv_p.at[part, slot], p_send.at[part, k], p_recv.at[part, slot], (me, to)
        )

    for part in range(CHUNKS):
        p_copy(part, col, 0, other).start()

    @pl.when(core == 1)
    def _():
        for part in range(CHUNKS):
            p_copy(part, col, 1, partner).start()

    @pl.when(core == 0)
    def _():
        for part in range(CHUNKS):
            recv_p[part, col] = send_p[part]

    @pl.when(me == 0)
    def _():
        for source in (partner, other, other + 1):
            x_copy(0, source, source).wait_recv()
        spread_out(norm(recv_x), 0, 2)

    def n_copy(part):
        return remote(
            recv_n.at[part], recv_n.at[part], n_sem.at[0, part], n_sem.at[1, part], (me, partner)
        )

    @pl.when(core == 0)
    def _():
        for part in range(CHUNKS):
            for source in (partner, other, other + 1):
                p_copy(part, source, 0, source).wait_recv()
            normed = norm(recv_p[part])
            recv_n[part] = normed
            n_copy(part).start()
            spread_out(normed, 2 * me + 1 + part, part)

    @pl.when(core == 1)
    def _():
        for part in range(CHUNKS):
            n_copy(part).wait_recv()
            spread_out(recv_n[part], 2 * me + 1 + part, part)

    def attend(queries, keys, values):
        count, seen_before = queries.shape[0], keys.shape[0] - queries.shape[0]
        left = iota(queries.shape, 1) < lanes
        scaled = queries.astype(F32) * (lanes ** (-0.5))
        heads_apart = [jnp.where(left, scaled, 0.0), jnp.where(left, 0.0, scaled)]
        stacked = jnp.concatenate(heads_apart, axis=0).astype(BF16)
        scores = fast_dot(stacked, keys, ((1,), (1,)))
        corner = (2 * count, count)
        row = iota(corner, 0)
        row = jnp.where(row < count, row, row - count)
        last = jnp.where(row >= iota(corner, 1), scores[:, seen_before:], -1e30)
        highest = jnp.max(last, axis=-1, keepdims=True)
        if seen_before:
            first = scores[:, :seen_before]
            highest = jnp.maximum(highest, jnp.max(first, axis=-1, keepdims=True))
        exps = jnp.exp(last - highest)
        total = jnp.sum(exps, axis=-1, keepdims=True)
        result = fast_dot(exps.astype(BF16), values[seen_before:])
        if seen_before:
            exps = jnp.exp(first - highest)
            total = total + jnp.sum(exps, axis=-1, keepdims=True)
            result = result + fast_dot(exps.astype(BF16), values[:seen_before])
        result = result / total
        return jnp.where(left, result[:count], result[count:]).astype(BF16)

    @pl.when(me == 0)
    def _():
        for pair in range(pairs):
            q, k, v = [
                jnp.concatenate([send_q[pair, 2, i], send_q[pair, 0, i]], axis=0) for i in range(3)
            ]
            first_out[:, pair * pair_width : (pair + 1) * pair_width] = attend(q, k, v)
        pltpu.make_async_copy(first_out, out_ref, out_sem).start()

    def o_copy(s, j):
        place = pl.ds(pl.multiple_of(j * pair_width, pair_width), pair_width)
        return remote(send_o.at[s], out_ref.at[:, place], o_send.at[s], o_recv.at[j], (s, col))

    def o_keep(j):
        place = pl.ds(pl.multiple_of(j * pair_width, pair_width), pair_width)
        return pltpu.make_async_copy(send_o.at[me], out_ref.at[:, place], out_sem)

    @pl.when(is_owner)
    def _():
        mine = me - lo
        for part in range(CHUNKS):
            recv_q[2 * me + 1 + part] = send_q[mine, part]
        span = 2 * rows
        step = span // half
        arrived = 0
        for n in range(seqs // 2):
            for block in range(arrived, step * (n + 1)):

                @pl.when(me != max(block - 1, 0) // 2)
                def _():
                    q_copy(mine, block, 0).wait_recv()

            arrived = max(arrived, step * (n + 1))
            q = recv_q[step * n : step * (n + 1), 0].reshape(span, pair_width)
            k, v = [recv_q[: step * (n + 1), i].reshape((n + 1) * span, pair_width) for i in (1, 2)]
            result = attend(q, k, v)
            for s in (2 * n, 2 * n + 1):
                if s == 0:
                    continue
                send_o[s] = result[(s - 2 * n) * rows : (s - 2 * n + 1) * rows]

                @pl.when(me != s)
                def _():
                    o_copy(s, mine).start()

        o_keep(mine).start()
        o_keep(mine).wait()

    @pl.when(me == 0)
    def _():
        pltpu.make_async_copy(first_out, out_ref, out_sem).wait()

    for j in range(pairs):

        @pl.when((me > 0) & (me != lo + j))
        def _():
            o_copy(me, j).wait_recv()

    for part in range(CHUNKS):
        p_copy(part, col, 0, other).wait_send()

        @pl.when(core == 1)
        def _():
            p_copy(part, col, 1, partner).wait_send()

        @pl.when(core == 0)
        def _():
            n_copy(part).wait_send()

    @pl.when(has_below)
    def _():
        w_copy.wait_send()

    @pl.when(me == 0)
    def _():
        for k in range(3):
            x_copy(k, col, partner).wait_send()
        for j in range(pairs):
            q_copy(j, 0, 2).wait_send()

    for j in range(pairs):

        @pl.when((me != lo + j) & (me < seqs - 1))
        def _():
            a_copy(j, me).wait_send()

        @pl.when(me != lo + j)
        def _():
            q_copy(j, 0, 0).wait_send()

        @pl.when((me != lo + j) & has_above)
        def _():
            q_copy(j, 0, 1).wait_send()

    for to in targets:
        tag_copy(to, me, me).wait_send()

    for s in range(1, seqs):

        @pl.when(is_owner & (me != s))
        def _():
            b_copy(s, me - lo).wait_send()
            o_copy(s, me - lo).wait_send()


def fused_body(
    byte_input,
    b_proj,
    c_proj,
    step_decay,
    skip_gain,
    out_weight,
    boundaries,
    counts,
    norm_gain,
    qkv_weight,
):
    seqs, groups = lax.axis_size("seq"), lax.axis_size("head")
    heads = step_decay.shape[0]
    length, width = byte_input.shape
    lanes = width // heads
    pairs = heads // 2
    state = b_proj.shape[1]
    rows = ROWS_DEV
    half = rows // 2
    enc = out_weight.shape[1]
    hbm = pl.BlockSpec(memory_space=pl.ANY)
    dma = pltpu.SemaphoreType.DMA
    operands = (
        step_decay,
        byte_input,
        b_proj,
        counts.reshape(1, 1),
        boundaries,
        c_proj,
        skip_gain.reshape(1, -1),
        out_weight,
        norm_gain.reshape(1, -1),
        qkv_weight,
    )
    result = pl.pallas_call(
        functools.partial(fused, seqs, groups),
        out_shape=jax.ShapeDtypeStruct((rows, width), BF16),
        in_specs=[hbm] * len(operands),
        out_specs=hbm,
        scratch_shapes=[pltpu.VMEM(array.shape, array.dtype) for array in operands]
        + [
            pltpu.VMEM((pairs, length, 4 * lanes), BF16),
            pltpu.VMEM((1, state), F32),
            pltpu.VMEM((seqs, 1, state), F32),
            pltpu.VMEM((pairs, state, 2 * lanes), BF16),
            pltpu.VMEM((seqs, state, 2 * lanes), BF16),
            pltpu.VMEM((seqs, state, 2 * lanes), BF16),
            pltpu.VMEM((pairs, state, 2 * lanes), BF16),
            pltpu.VMEM((rows, width + 3 * state), BF16),
            pltpu.VMEM((rows, width + 3 * state), BF16),
            pltpu.VMEM((half, enc), BF16),
            pltpu.VMEM((groups, half, enc), BF16),
            pltpu.VMEM((CHUNKS, half, enc), BF16),
            pltpu.VMEM((CHUNKS, groups, half, enc), BF16),
            pltpu.VMEM((CHUNKS, half, enc), BF16),
            pltpu.VMEM((pairs, CHUNKS + 1, 3, half, 2 * lanes), BF16),
            pltpu.VMEM((seqs * CHUNKS, 3, half, 2 * lanes), BF16),
            pltpu.VMEM((seqs, rows, 2 * lanes), BF16),
            pltpu.VMEM((rows, width), BF16),
            dma((len(operands),)),
            dma((2, seqs)),
            dma((pairs,)),
            dma((seqs,)),
            dma((seqs,)),
            dma((pairs,)),
            dma((2,)),
            dma((groups,)),
            dma((groups,)),
            dma((CHUNKS, 2)),
            dma((CHUNKS, groups)),
            dma((2, CHUNKS)),
            dma((CHUNKS + 1, pairs)),
            dma((CHUNKS * seqs,)),
            dma((seqs,)),
            dma((pairs,)),
            dma,
        ],
        compiler_params=pltpu.CompilerParams(collective_id=0, has_side_effects=True),
    )(*operands)
    return result.astype(F32)


def chosen(*args):
    byte_input, step_decay, slots = args[0], args[3], args[6].shape[1]
    heads = step_decay.shape[0]
    lanes = byte_input.shape[1] // heads
    seqs, groups = lax.axis_size("seq"), lax.axis_size("head")
    fits = seqs == heads and lanes == ATT_DIM and args[9].shape[2] == byte_input.shape[1]
    fits = fits and 2 * lanes == slots and args[1].shape[1] == slots and slots == 2 * ROWS_DEV
    fits = fits and seqs % 4 == 0 and groups == 2 * CHUNKS and ROWS_DEV % (16 * groups) == 0
    fits = fits and byte_input.shape[0] % slots == 0
    return fused_body(*args) if fits else body(*args)


def solution(mesh):
    return jax.shard_map(
        chosen,
        mesh=mesh,
        in_specs=(
            P("seq", "head"),
            P("seq", None),
            P("seq", None),
            P("head", "seq"),
            P("head"),
            P("head", None),
            P("seq", None),
            P("seq"),
            P(),
            P(None, None, "head"),
        ),
        out_specs=P("seq", "head"),
        check_vma=False,
    )
```

```python
import functools

import jax
import jax.numpy as jnp
from jax import lax
from jax.experimental import pallas as pl
from jax.experimental.pallas import tpu as pltpu
from jax.sharding import PartitionSpec as P

ATT_DIM = 64
ROWS_DEV = 64


def prefix(shard, axis, combine, identity):
    length, here = (lax.axis_size(axis), lax.axis_index(axis))
    everything = jax.tree.map(lambda part: lax.all_gather(part, axis), shard)
    start = jax.tree.map(
        lambda part, zero: jnp.broadcast_to(jnp.asarray(zero, part.dtype), part.shape),
        shard,
        identity,
    )

    def lap(k, before):
        reached = k < here
        new = combine(before, jax.tree.map(lambda part: part[k], everything))
        return jax.tree.map(lambda a, b: jnp.where(reached, a, b), new, before)

    return lax.fori_loop(0, length, lap, start)


def extended(cells, sides, width):
    for axis, dim in sides:
        count = lax.axis_size(axis)
        ends = count - 1
        head = lax.slice_in_dim(cells, 0, width, axis=dim)
        tail = lax.slice_in_dim(cells, cells.shape[dim] - width, cells.shape[dim], axis=dim)
        cells = jnp.concatenate(
            [
                lax.ppermute(tail, axis, [(i, (i + 1) % count) for i in range(ends)]),
                cells,
                lax.ppermute(head, axis, [((i + 1) % count, i) for i in range(ends)]),
            ],
            axis=dim,
        )
    return cells


def state_space(inputs, b_rows, c_rows, decay):
    log_decay = jnp.cumsum(-decay, axis=1)
    affinity = jnp.dot(c_rows, b_rows.T, precision=lax.Precision.HIGHEST)
    length = inputs.shape[0]
    causal = lax.broadcasted_iota(jnp.int32, (length, length), 0) >= lax.broadcasted_iota(
        jnp.int32, (length, length), 1
    )

    def one_head(pair):
        values, logs = pair
        weights = (
            jnp.where(causal, jnp.exp(jnp.where(causal, logs[:, None] - logs[None, :], 0.0)), 0.0)
            * affinity
        )
        return jnp.dot(weights, values, precision=lax.Precision.HIGHEST)

    inside = lax.map(one_head, (inputs.transpose(1, 0, 2), log_decay))
    tail = jnp.exp(log_decay[:, -1:] - log_decay)
    own_state = jnp.einsum("ht,thp,tn->hpn", tail, inputs, b_rows, precision=lax.Precision.HIGHEST)
    return (log_decay, inside, own_state)


def link(earlier, later):
    return (earlier[0] * later[0], later[0][:, None, None] * earlier[1] + later[1])


def body(
    byte_input,
    b_proj,
    c_proj,
    step_decay,
    skip_gain,
    out_weight,
    boundaries,
    counts,
    norm_gain,
    qkv_weight,
):
    heads_here = step_decay.shape[0]
    length = byte_input.shape[0]
    inputs = byte_input.reshape(length, heads_here, -1)
    log_decay, inside, own_state = state_space(inputs, b_proj, c_proj, step_decay)
    span_decay = jnp.exp(log_decay[:, -1])
    arriving = prefix(
        (span_decay, own_state), "seq", link, (jnp.ones_like(span_decay), jnp.zeros_like(own_state))
    )
    carried = jnp.exp(log_decay)[:, :, None] * jnp.einsum(
        "tn,hpn->htp", c_proj, arriving[1], precision=lax.Precision.HIGHEST
    )
    mixed_heads = inside + carried + skip_gain[:, None, None] * inputs.transpose(1, 0, 2)
    slots = boundaries.shape[1]
    picked = jnp.take(mixed_heads, boundaries[0], axis=1)
    selected = picked.transpose(1, 0, 2).reshape(slots, -1).astype(jnp.bfloat16)
    all_counts = lax.all_gather(counts, "seq", axis=0, tiled=True)
    starts = jnp.cumsum(all_counts) - all_counts
    myself = lax.axis_index("seq")
    shards = lax.axis_size("seq")
    slot = jnp.arange(slots, dtype=jnp.int32)

    def slot_index(source):
        inside_axis = (source >= 0) & (source < shards)
        safe = jnp.clip(source, 0, shards - 1)
        begin = jnp.take(starts, safe)
        number = jnp.take(all_counts, safe)
        return jnp.where(inside_axis & (slot < number), begin + slot, -1)

    global_index = jnp.concatenate(
        [slot_index(myself - 1), slot_index(myself), slot_index(myself + 1)]
    )
    first_row = myself * ROWS_DEV
    target = first_row + jnp.arange(ROWS_DEV, dtype=jnp.int32)
    picker = global_index[None, :] == target[:, None]
    nearby = extended(selected, (("seq", 0),), slots)
    owned = jnp.dot(picker.astype(jnp.bfloat16), nearby, preferred_element_type=jnp.float32).astype(
        jnp.bfloat16
    )
    partial_value = jnp.dot(owned, out_weight, preferred_element_type=jnp.float32)
    packed = lax.psum(partial_value, "head")
    normed = (
        packed * lax.rsqrt(jnp.mean(packed * packed, axis=-1, keepdims=True) + 1e-05) * norm_gain
    ).astype(jnp.bfloat16)
    query = jnp.dot(normed, qkv_weight[0], preferred_element_type=jnp.float32).astype(jnp.bfloat16)
    keyed = jnp.dot(normed, qkv_weight[1], preferred_element_type=jnp.float32).astype(jnp.bfloat16)
    valued = jnp.dot(normed, qkv_weight[2], preferred_element_type=jnp.float32).astype(jnp.bfloat16)
    att_here = query.shape[1] // ATT_DIM
    queries = query.reshape(ROWS_DEV, att_here, ATT_DIM)
    row_place = first_row + jnp.arange(ROWS_DEV, dtype=jnp.int32)
    scale = ATT_DIM ** (-0.5)
    running = jnp.full((att_here, ROWS_DEV), -1e30, jnp.float32)
    key_piece = lax.all_gather(keyed, "seq", axis=0, tiled=True)
    value_piece = lax.all_gather(valued, "seq", axis=0, tiled=True)
    count = key_piece.shape[0]
    key_heads = key_piece.reshape(count, att_here, ATT_DIM)
    value_heads = value_piece.reshape(count, att_here, ATT_DIM)
    scores = (
        jnp.einsum("qhd,khd->hqk", queries, key_heads, preferred_element_type=jnp.float32) * scale
    )
    allowed = jnp.arange(count, dtype=jnp.int32)[None, :] <= row_place[:, None]
    scores = jnp.where(allowed[None], scores, -1e30)
    highest = jnp.maximum(running, jnp.max(scores, axis=-1))
    exps = jnp.where(allowed[None], jnp.exp(scores - highest[:, :, None]), 0.0)
    totals = jnp.sum(exps, axis=-1)
    weights = exps.astype(jnp.bfloat16)
    accum = jnp.einsum("hqk,khd->hqd", weights, value_heads, preferred_element_type=jnp.float32)
    running, totals, accum = (highest, totals, accum)
    result = accum / totals[:, :, None]
    return result.transpose(1, 0, 2).reshape(ROWS_DEV, att_here * ATT_DIM)


F32 = jnp.float32
BF16 = jnp.bfloat16
CHUNKS = 2


def exact_dot(a, b, dims=((1,), (0,))):
    return lax.dot_general(
        a, b, (dims, ((), ())), precision=lax.Precision.HIGHEST, preferred_element_type=F32
    )


def fast_dot(a, b, dims=((1,), (0,))):
    return lax.dot_general(a, b, (dims, ((), ())), preferred_element_type=F32)


def halves(a):
    high = a.astype(BF16)
    return high, (a - high.astype(F32)).astype(BF16)


def iota(shape, dim):
    return lax.broadcasted_iota(jnp.int32, shape, dim)


def fused(
    seqs,
    groups,
    decay_hbm,
    x_hbm,
    b_hbm,
    counts_hbm,
    bound_hbm,
    c_hbm,
    skip_hbm,
    outw_hbm,
    gain_hbm,
    qkvw_hbm,
    out_ref,
    decay_ref,
    x_ref,
    b_ref,
    counts_ref,
    bound_ref,
    c_ref,
    skip_ref,
    outw,
    gain_ref,
    qkvw,
    x_both,
    tag_send,
    tag_recv,
    send_a,
    recv_a,
    send_b,
    recv_b,
    send_w,
    recv_w,
    send_x,
    recv_x,
    send_p,
    recv_p,
    recv_n,
    send_q,
    recv_q,
    send_o,
    first_out,
    weight_sem,
    tag_sem,
    a_send,
    a_recv,
    b_send,
    b_recv,
    w_sem,
    x_send,
    x_recv,
    p_send,
    p_recv,
    n_sem,
    q_send,
    q_recv,
    o_send,
    o_recv,
    out_sem,
):
    me = lax.axis_index("seq")
    col = lax.axis_index("head")
    length, width = x_ref.shape
    heads = decay_ref.shape[0]
    lanes = width // heads
    pair_width = 2 * lanes
    pairs = heads // 2
    state = b_ref.shape[1]
    slots = bound_ref.shape[1]
    rows = out_ref.shape[0]
    half = rows // 2
    lo = (seqs - pairs) // 2
    is_owner = (me >= lo) & (me < lo + pairs)
    has_below, has_above = me > 0, me < seqs - 1

    def shard_at(d):
        return lax.rem(me + d + seqs, seqs)

    layers = seqs // 2
    mid = layers // 2
    layer, side = me // 2, lax.rem(me, 2)
    near_end = layer < mid
    far_layers = [jnp.where(near_end, layers - 1 - k, k) for k in range(layers - mid)]
    same = jnp.where(near_end, layer, layer - (layers - mid))
    for k in range(1, mid):
        turn = lax.rem(same + k, mid)
        far_layers.append(jnp.where(near_end, turn, turn + (layers - mid)))
    targets = []
    for there in far_layers + [layer]:
        targets.append(2 * there + 1 - side)
        if there is not layer:
            targets.append(2 * there + side)

    def head_at(d):
        return lax.rem(col + d, groups)

    chip = col // 2
    core = lax.rem(col, 2)
    partner = 2 * chip + 1 - core
    other = 2 * (1 - chip)

    barrier = pltpu.get_barrier_semaphore()
    peers = [(shard_at(d), col) for d in range(1, seqs)]
    peers += [(me, head_at(d)) for d in range(1, groups)]
    for peer in peers:
        pl.semaphore_signal(
            barrier, inc=1, device_id=peer, device_id_type=pl.DeviceIdType.MESH
        )

    def remote(src, dst, send_sem, recv_sem, peer):
        return pltpu.make_async_remote_copy(
            src_ref=src,
            dst_ref=dst,
            send_sem=send_sem,
            recv_sem=recv_sem,
            device_id=peer,
            device_id_type=pl.DeviceIdType.MESH,
        )

    loads = [
        pltpu.make_async_copy(source, target, weight_sem.at[i])
        for i, (source, target) in enumerate(
            (
                (decay_hbm, decay_ref),
                (x_hbm, x_ref),
                (b_hbm, b_ref),
                (counts_hbm, counts_ref),
                (bound_hbm, bound_ref),
                (c_hbm, c_ref),
                (skip_hbm, skip_ref),
                (outw_hbm, outw),
                (gain_hbm, gain_ref),
                (qkvw_hbm, qkvw),
            )
        )
    ]
    for load in loads[:7]:
        load.start()

    loads[0].wait()
    decay = decay_ref[...]
    upper = (iota((length, length), 0) <= iota((length, length), 1)).astype(F32)
    logs = -exact_dot(decay, upper)
    tail = jnp.exp(logs[:, length - 1 : length] - logs)
    loads[3].wait()
    tag_row = iota((heads, state), 1) == iota((heads, state), 0)
    tags = jnp.where(tag_row, logs[:, length - 1 : length], 0.0)
    tags = jnp.sum(tags, axis=0, keepdims=True)
    number = jnp.broadcast_to(counts_ref[...].astype(F32), (1, state))
    tag_send[...] = jnp.where(iota((1, state), 1) == heads, number, tags)
    loads[1].wait()
    loads[2].wait()
    for load in loads[7:]:
        load.start()
    b_turned = b_ref[...].T
    first_half = iota((state, pair_width), 1) < lanes
    for pair in range(pairs):
        x_high, x_low = halves(x_ref[:, pair * pair_width : (pair + 1) * pair_width])
        both = jnp.concatenate([x_high, x_low], axis=1)
        x_both[pair] = both
        faded = [b_turned * tail[h : h + 1, :] for h in (2 * pair, 2 * pair + 1)]
        f_high, f_low = halves(jnp.concatenate(faded, axis=0))
        wide = fast_dot(f_high, both)
        own = wide[:, :pair_width] + wide[:, pair_width:] + fast_dot(f_low, x_high)
        send_a[pair] = jnp.where(first_half, own[:state], own[state:]).astype(BF16)
    pl.semaphore_wait(barrier, len(peers))

    def tag_copy(to, slot, source):
        return remote(tag_send, tag_recv.at[slot], tag_sem.at[0, to], tag_sem.at[1, source], (to, col))

    def a_copy(j, slot):
        return remote(send_a.at[j], recv_a.at[slot], a_send.at[j], a_recv.at[slot], (lo + j, col))

    for to in targets:
        tag_copy(to, me, me).start()
    for k in range(pairs):
        j = jnp.where(near_end, pairs - 1 - k, k)

        @pl.when((me != lo + j) & (me < seqs - 1))
        def _():
            a_copy(j, me).start()

    tag_recv[me] = tag_send[...]

    @pl.when(is_owner)
    def _():
        recv_a[me] = send_a[me - lo]

    @pl.when(me == 0)
    def _():
        recv_b[...] = jnp.zeros(recv_b.shape, recv_b.dtype)

    lower = (iota((length, length), 0) >= iota((length, length), 1)).astype(F32)
    twice = [decay, decay, jnp.zeros((state - 2 * heads, length), F32)]
    logs_t = -exact_dot(lower, jnp.concatenate(twice, axis=0), ((1,), (1,)))
    lane = iota((state, width), 0)
    first = lax.rem(lane, heads) * lanes
    channel = iota((state, width), 1)
    spread = (channel >= first) & (channel < first + lanes)
    spread_one = (spread & (lane < heads)).astype(F32)
    spread_two = (spread & (lane < 2 * heads)).astype(BF16)
    for load in loads[4:7]:
        load.wait()
    marks = jnp.broadcast_to(bound_ref[...].astype(F32), (slots, slots)).T
    marks = jnp.concatenate([marks] * (length // slots), axis=1)
    place = iota((slots, length), 1).astype(F32)
    hit = place == marks
    seen = place <= marks
    onehot = hit.astype(F32)
    c_rows = exact_dot(onehot, c_ref[...])
    logs_sel = exact_dot(onehot, logs_t)
    affinity = exact_dot(c_rows, b_ref[...], ((1,), (1,)))
    inside = []
    first_lane = iota((slots, pair_width), 1) < lanes
    for pair in range(pairs):
        both = x_both[pair]
        parts = []
        for h in (2 * pair, 2 * pair + 1):
            gap = logs_sel[:, h : h + 1] - logs[h : h + 1, :]
            weights = jnp.where(seen, jnp.exp(jnp.where(seen, gap, 0.0)), 0.0) * affinity
            weights = weights + jnp.where(hit, skip_ref[:, h : h + 1], 0.0)
            w_high, w_low = halves(weights)
            wide = fast_dot(w_high, both)
            parts.append(
                wide[:, :pair_width] + wide[:, pair_width:] + fast_dot(w_low, both[:, :pair_width])
            )
        inside.append(jnp.where(first_lane, parts[0], parts[1]))
    inside = jnp.concatenate(inside, axis=1)
    enter = jnp.exp(logs_sel)
    e_high = enter.astype(BF16).astype(F32)
    enter_lane = iota((slots, state), 1)
    e_pack = jnp.where(enter_lane < heads, e_high, enter - e_high)
    e_pack = jnp.where(enter_lane < 2 * heads, e_pack, 0.0).astype(BF16)
    sel = jnp.concatenate([*halves(inside), *halves(c_rows), e_pack], axis=1)

    for d in range(1, seqs):
        source = shard_at(-d)
        tag_copy(shard_at(d), source, source).wait_recv()
    all_tags = tag_recv[...].reshape(seqs, state)
    tag_lane = iota((seqs, state), 1)
    tag_shard = iota((seqs, state), 0)
    earlier = (tag_shard < me) & (tag_lane == heads)
    start = jnp.sum(jnp.where(earlier, all_tags, 0.0), axis=(0, 1), keepdims=True)
    offset = start - (me * rows - half).astype(F32)
    slot = iota((slots, slots), 1).astype(F32)
    count = jnp.broadcast_to(counts_ref[...].astype(F32), (slots, slots))
    shift = (slot == iota((slots, slots), 0).astype(F32) - offset) & (slot < count)
    shift = shift.astype(BF16)
    passed = jnp.concatenate([sel[:, :width], sel[:, 2 * width :]], axis=1)
    send_w[...] = fast_dot(shift[:rows], passed).astype(BF16)

    w_copy = remote(send_w, recv_w, w_sem.at[0], w_sem.at[1], (shard_at(-1), col))

    @pl.when(has_below)
    def _():
        w_copy.start()

    @pl.when(jnp.logical_not(has_above))
    def _():
        recv_w[...] = jnp.zeros(recv_w.shape, recv_w.dtype)

    for load in loads[7:]:
        load.wait()

    def norm(parts):
        mixed = parts[0].astype(F32)
        for k in range(1, groups):
            mixed = mixed + parts[k].astype(F32)
        square = jnp.mean(mixed * mixed, axis=-1, keepdims=True)
        return (mixed * lax.rsqrt(square + 1e-05) * gain_ref[...]).astype(BF16)

    def q_copy(j, block, part):
        return remote(
            send_q.at[j, part], recv_q.at[block], q_send.at[part, j], q_recv.at[block], (lo + j, col)
        )

    def spread_out(block, to, part):
        for i in range(3):
            product = fast_dot(block, qkvw[i]).astype(BF16)
            for pair in range(pairs):
                send_q[pair, part, i] = product[:, pair * pair_width : (pair + 1) * pair_width]
        for k in range(pairs):
            j = jnp.where(near_end, pairs - 1 - k, k)

            @pl.when((me != lo + j) & (to < 2 * seqs))
            def _():
                q_copy(j, to, part).start()

    def x_copy(k, slot, to):
        return remote(send_x, recv_x.at[slot], x_send.at[k], x_recv.at[slot], (me, to))

    @pl.when(me == 0)
    def _():
        early = fast_dot(shift[half:rows], sel[:, : 2 * width])
        early = early[:, :width] + early[:, width:]
        send_x[...] = fast_dot(early.astype(BF16), outw[...]).astype(BF16)
        for k, to in enumerate((other, other + 1, partner)):
            x_copy(k, col, to).start()
        recv_x[col] = send_x[...]

    owned = fast_dot(shift[rows:], sel)

    def b_copy(s, j):
        return remote(send_b.at[s], recv_b.at[j], b_send.at[s], b_recv.at[j], (s, col))

    @pl.when(is_owner)
    def _():
        mine = me - lo
        even = jnp.sum(jnp.where(tag_lane == 2 * mine, all_tags, 0.0), axis=1, keepdims=True)
        odd = jnp.sum(jnp.where(tag_lane == 2 * mine + 1, all_tags, 0.0), axis=1, keepdims=True)
        kept = jnp.exp(jnp.where(iota((seqs, pair_width), 1) < lanes, even, odd))
        running = jnp.zeros((state, pair_width), F32)
        for s in range(1, seqs):

            @pl.when(me != s - 1)
            def _():
                a_copy(mine, s - 1).wait_recv()

            running = kept[s - 1 : s] * running + recv_a[s - 1].astype(F32)
            send_b[s] = running.astype(BF16)

            @pl.when(me != s)
            def _():
                b_copy(s, mine).start()

        recv_b[mine] = send_b[me]

    spans = jnp.exp(jnp.where(tag_lane < heads, all_tags, 0.0))
    here = jnp.sum(jnp.where(tag_shard == me, spans, 0.0), axis=0, keepdims=True)
    span_here = exact_dot(jnp.broadcast_to(here, (heads, state)), spread_one)[0:1]
    mine_scale = fast_dot(owned[:, 2 * width + 2 * state :].astype(BF16), spread_two)

    @pl.when(has_above)
    def _():
        w_copy.wait_recv()

    near_rows = recv_w[...].astype(F32)
    near_scale = fast_dot(recv_w[:, width + 2 * state :], spread_two)
    c_both = owned[:, 2 * width : 2 * width + 2 * state] + near_rows[:, width : width + 2 * state]
    c_stack = jnp.concatenate([c_both[:, :state], c_both[:, state:]], axis=0).astype(BF16)

    def through(ref):
        wide = fast_dot(c_stack, jnp.concatenate([ref[j] for j in range(pairs)], axis=1))
        return wide[:rows] + wide[rows:]

    reach = owned[:, :width] + owned[:, width : 2 * width] + near_rows[:, :width]
    reach = reach + near_scale * through(send_a)
    far_scale = mine_scale + span_here * near_scale

    for j in range(pairs):

        @pl.when(has_below & (me != lo + j))
        def _():
            b_copy(me, j).wait_recv()

    y = (reach + far_scale * through(recv_b)).astype(BF16)
    partial = fast_dot(y, outw[...]).astype(BF16)
    for part in range(CHUNKS):
        send_p[part] = partial[part * half : (part + 1) * half]

    def p_copy(part, slot, k, to):
        return remote(
            send_p.at[part], recv_p.at[part, slot], p_send.at[part, k], p_recv.at[part, slot], (me, to)
        )

    for part in range(CHUNKS):
        p_copy(part, col, 0, other).start()

    @pl.when(core == 1)
    def _():
        for part in range(CHUNKS):
            p_copy(part, col, 1, partner).start()

    @pl.when(core == 0)
    def _():
        for part in range(CHUNKS):
            recv_p[part, col] = send_p[part]

    @pl.when(me == 0)
    def _():
        for source in (partner, other, other + 1):
            x_copy(0, source, source).wait_recv()
        spread_out(norm(recv_x), 0, 2)

    def n_copy(part):
        return remote(
            recv_n.at[part], recv_n.at[part], n_sem.at[0, part], n_sem.at[1, part], (me, partner)
        )

    @pl.when(core == 0)
    def _():
        for part in range(CHUNKS):
            for source in (partner, other, other + 1):
                p_copy(part, source, 0, source).wait_recv()
            normed = norm(recv_p[part])
            recv_n[part] = normed
            n_copy(part).start()
            spread_out(normed, 2 * me + 1 + part, part)

    @pl.when(core == 1)
    def _():
        for part in range(CHUNKS):
            n_copy(part).wait_recv()
            spread_out(recv_n[part], 2 * me + 1 + part, part)

    def attend(queries, keys, values):
        count, seen_before = queries.shape[0], keys.shape[0] - queries.shape[0]
        left = iota(queries.shape, 1) < lanes
        scaled = queries.astype(F32) * (lanes ** (-0.5))
        heads_apart = [jnp.where(left, scaled, 0.0), jnp.where(left, 0.0, scaled)]
        stacked = jnp.concatenate(heads_apart, axis=0).astype(BF16)
        scores = fast_dot(stacked, keys, ((1,), (1,)))
        corner = (2 * count, count)
        row = iota(corner, 0)
        row = jnp.where(row < count, row, row - count)
        last = jnp.where(row >= iota(corner, 1), scores[:, seen_before:], -1e30)
        highest = jnp.max(last, axis=-1, keepdims=True)
        if seen_before:
            first = scores[:, :seen_before]
            highest = jnp.maximum(highest, jnp.max(first, axis=-1, keepdims=True))
        exps = jnp.exp(last - highest)
        total = jnp.sum(exps, axis=-1, keepdims=True)
        result = fast_dot(exps.astype(BF16), values[seen_before:])
        if seen_before:
            exps = jnp.exp(first - highest)
            total = total + jnp.sum(exps, axis=-1, keepdims=True)
            result = result + fast_dot(exps.astype(BF16), values[:seen_before])
        result = result / total
        return jnp.where(left, result[:count], result[count:]).astype(BF16)

    @pl.when(me == 0)
    def _():
        for pair in range(pairs):
            q, k, v = [
                jnp.concatenate([send_q[pair, 2, i], send_q[pair, 0, i]], axis=0) for i in range(3)
            ]
            first_out[:, pair * pair_width : (pair + 1) * pair_width] = attend(q, k, v)
        pltpu.make_async_copy(first_out, out_ref, out_sem).start()

    def o_copy(s, j):
        place = pl.ds(pl.multiple_of(j * pair_width, pair_width), pair_width)
        return remote(send_o.at[s], out_ref.at[:, place], o_send.at[s], o_recv.at[j], (s, col))

    def o_keep(j):
        place = pl.ds(pl.multiple_of(j * pair_width, pair_width), pair_width)
        return pltpu.make_async_copy(send_o.at[me], out_ref.at[:, place], out_sem)

    @pl.when(is_owner)
    def _():
        mine = me - lo
        for part in range(CHUNKS):
            recv_q[2 * me + 1 + part] = send_q[mine, part]
        span = 2 * rows
        step = span // half
        arrived = 0
        for n in range(seqs // 2):
            for block in range(arrived, step * (n + 1)):

                @pl.when(me != max(block - 1, 0) // 2)
                def _():
                    q_copy(mine, block, 0).wait_recv()

            arrived = max(arrived, step * (n + 1))
            q = recv_q[step * n : step * (n + 1), 0].reshape(span, pair_width)
            k, v = [recv_q[: step * (n + 1), i].reshape((n + 1) * span, pair_width) for i in (1, 2)]
            result = attend(q, k, v)
            for s in (2 * n, 2 * n + 1):
                if s == 0:
                    continue
                send_o[s] = result[(s - 2 * n) * rows : (s - 2 * n + 1) * rows]

                @pl.when(me != s)
                def _():
                    o_copy(s, mine).start()

        o_keep(mine).start()
        o_keep(mine).wait()

    @pl.when(me == 0)
    def _():
        pltpu.make_async_copy(first_out, out_ref, out_sem).wait()

    for j in range(pairs):

        @pl.when((me > 0) & (me != lo + j))
        def _():
            o_copy(me, j).wait_recv()

    for part in range(CHUNKS):
        p_copy(part, col, 0, other).wait_send()

        @pl.when(core == 1)
        def _():
            p_copy(part, col, 1, partner).wait_send()

        @pl.when(core == 0)
        def _():
            n_copy(part).wait_send()

    @pl.when(has_below)
    def _():
        w_copy.wait_send()

    @pl.when(me == 0)
    def _():
        for k in range(3):
            x_copy(k, col, partner).wait_send()
        for j in range(pairs):
            q_copy(j, 0, 2).wait_send()

    for j in range(pairs):

        @pl.when((me != lo + j) & (me < seqs - 1))
        def _():
            a_copy(j, me).wait_send()

        @pl.when(me != lo + j)
        def _():
            q_copy(j, 0, 0).wait_send()

        @pl.when((me != lo + j) & has_above)
        def _():
            q_copy(j, 0, 1).wait_send()

    for to in targets:
        tag_copy(to, me, me).wait_send()

    for s in range(1, seqs):

        @pl.when(is_owner & (me != s))
        def _():
            b_copy(s, me - lo).wait_send()
            o_copy(s, me - lo).wait_send()


def fused_body(
    byte_input,
    b_proj,
    c_proj,
    step_decay,
    skip_gain,
    out_weight,
    boundaries,
    counts,
    norm_gain,
    qkv_weight,
):
    seqs, groups = lax.axis_size("seq"), lax.axis_size("head")
    heads = step_decay.shape[0]
    length, width = byte_input.shape
    lanes = width // heads
    pairs = heads // 2
    state = b_proj.shape[1]
    rows = ROWS_DEV
    half = rows // 2
    enc = out_weight.shape[1]
    hbm = pl.BlockSpec(memory_space=pl.ANY)
    dma = pltpu.SemaphoreType.DMA
    operands = (
        step_decay,
        byte_input,
        b_proj,
        counts.reshape(1, 1),
        boundaries,
        c_proj,
        skip_gain.reshape(1, -1),
        out_weight,
        norm_gain.reshape(1, -1),
        qkv_weight,
    )
    result = pl.pallas_call(
        functools.partial(fused, seqs, groups),
        out_shape=jax.ShapeDtypeStruct((rows, width), BF16),
        in_specs=[hbm] * len(operands),
        out_specs=hbm,
        scratch_shapes=[pltpu.VMEM(array.shape, array.dtype) for array in operands]
        + [
            pltpu.VMEM((pairs, length, 4 * lanes), BF16),
            pltpu.VMEM((1, state), F32),
            pltpu.VMEM((seqs, 1, state), F32),
            pltpu.VMEM((pairs, state, 2 * lanes), BF16),
            pltpu.VMEM((seqs, state, 2 * lanes), BF16),
            pltpu.VMEM((seqs, state, 2 * lanes), BF16),
            pltpu.VMEM((pairs, state, 2 * lanes), BF16),
            pltpu.VMEM((rows, width + 3 * state), BF16),
            pltpu.VMEM((rows, width + 3 * state), BF16),
            pltpu.VMEM((half, enc), BF16),
            pltpu.VMEM((groups, half, enc), BF16),
            pltpu.VMEM((CHUNKS, half, enc), BF16),
            pltpu.VMEM((CHUNKS, groups, half, enc), BF16),
            pltpu.VMEM((CHUNKS, half, enc), BF16),
            pltpu.VMEM((pairs, CHUNKS + 1, 3, half, 2 * lanes), BF16),
            pltpu.VMEM((seqs * CHUNKS, 3, half, 2 * lanes), BF16),
            pltpu.VMEM((seqs, rows, 2 * lanes), BF16),
            pltpu.VMEM((rows, width), BF16),
            dma((len(operands),)),
            dma((2, seqs)),
            dma((pairs,)),
            dma((seqs,)),
            dma((seqs,)),
            dma((pairs,)),
            dma((2,)),
            dma((groups,)),
            dma((groups,)),
            dma((CHUNKS, 2)),
            dma((CHUNKS, groups)),
            dma((2, CHUNKS)),
            dma((CHUNKS + 1, pairs)),
            dma((CHUNKS * seqs,)),
            dma((seqs,)),
            dma((pairs,)),
            dma,
        ],
        compiler_params=pltpu.CompilerParams(collective_id=0, has_side_effects=True),
    )(*operands)
    return result.astype(F32)


def chosen(*args):
    byte_input, step_decay, slots = args[0], args[3], args[6].shape[1]
    heads = step_decay.shape[0]
    lanes = byte_input.shape[1] // heads
    seqs, groups = lax.axis_size("seq"), lax.axis_size("head")
    fits = seqs == heads and lanes == ATT_DIM and args[9].shape[2] == byte_input.shape[1]
    fits = fits and 2 * lanes == slots and args[1].shape[1] == slots and slots == 2 * ROWS_DEV
    fits = fits and seqs % 4 == 0 and groups == 2 * CHUNKS and ROWS_DEV % (16 * groups) == 0
    fits = fits and byte_input.shape[0] % slots == 0
    return fused_body(*args) if fits else body(*args)


def solution(mesh):
    return jax.shard_map(
        chosen,
        mesh=mesh,
        in_specs=(
            P("seq", "head"),
            P("seq", None),
            P("seq", None),
            P("head", "seq"),
            P("head"),
            P("head", None),
            P("seq", None),
            P("seq"),
            P(),
            P(None, None, "head"),
        ),
        out_specs=P("seq", "head"),
        check_vma=False,
    )
```
